128 devices in a mesh: cat: 2 (over x_hi), lat: 4 (over x_lo, core), lon: 16 (over z, y).
Axes of the slice: x: 4 (x_hi: 2, x_lo: 2; x = x_hi * 2 + x_lo), y: 4, z: 4, core: 2. Of those that a mesh axis runs over, the one named last changes fastest.
Arguments:
- thickness: bfloat16 [40, 1024, 10240], P('cat', 'lat', 'lon'), may hold values from 0.099609375 to 4
- area: bfloat16 [40, 1024, 10240], P('cat', 'lat', 'lon'), may hold values from 0.0049743652 to 0.049804688
- ridge_weight: float32 [40], P('cat'), may hold values from 0.2 to 2
- cat_top: int32 [1024, 10240], P('lat', 'lon'), may hold values from 1 to 40
- land_mask: int32 [1024, 10240], P('lat', 'lon'), may hold values 0 or 1
- velocity_u: float32 [1024, 10240], P('lat', 'lon'), may hold values from -1.8 to 1.8
- velocity_v: float32 [1024, 10240], P('lat', 'lon'), may hold values from -1.8 to 1.8
- stress_div: float32 [1024, 10240], P('lat', 'lon'), may hold values from -3 to 3
- stress_ten: float32 [1024, 10240], P('lat', 'lon'), may hold values from -3 to 3
- stress_shear: float32 [1024, 10240], P('lat', 'lon'), may hold values from -3 to 3
- wind_x: float32 [1024, 10240], P('lat', 'lon'), may hold values from -6 to 6
- wind_y: float32 [1024, 10240], P('lat', 'lon'), may hold values from -6 to 6
- water_drag: float32 [1024, 10240], P('lat', 'lon'), may hold values from 0.2 to 2
Outputs:
- new_u: float32 [1024, 10240], P('lat', 'lon')
- new_v: float32 [1024, 10240], P('lat', 'lon')
- new_div: float32 [1024, 10240], P('lat', 'lon')
- new_ten: float32 [1024, 10240], P('lat', 'lon')
- new_shear: float32 [1024, 10240], P('lat', 'lon')
The draws below stay inside these ranges and needn't reach their ends.
Inputs may be any that keep to these rules, and one draw needn't show every extreme that they name: Categories with index cat_top or above are absent from a cell.
All inputs are finite; a program needn't handle non-finite values. No bound on the sum of `land_mask` on one device may be relied on, other than what follows from the above.
Results may differ from the reference program's by a relative error of at most 0.0003.
Values sent between devices are 32-bit elements; how exact they have to be, the bound alone decides.
A program may use at most 128 MiB of HBM per device.

```python
import math
import jax
import jax.numpy as jnp
from jax import lax

NCAT = 40
SUB = 4
NLAT = 1024
NLON = 10240


def with_ends(entries, stream_key, least, high):
    shape = entries.shape
    spot = [jax.random.randint(jax.random.fold_in(stream_key, axis), (), 0, shape[axis]) for axis in range(len(shape))]
    entries = entries.at[tuple(spot)].set(least)
    longest = shape.index(max(shape))
    spot[longest] = (spot[longest] + 1) % shape[longest]
    return entries.at[tuple(spot)].set(high)


def shard_levels(rng, extent, cuts, low, high):
    factor_of = 1.0
    for axis_at, shards_of in cuts:
        steps = jax.random.uniform(jax.random.fold_in(jax.random.fold_in(rng, 6), axis_at), (shards_of,), jnp.float32, low / len(cuts), high / len(cuts))
        factor_of = factor_of * jnp.repeat(jnp.exp(steps), extent[axis_at] // shards_of).reshape((-1,) + (1,) * (len(extent) - 1 - axis_at))
    return factor_of


def noise(own_key, shape, deviation, limit, cuts=(), dtype=jnp.bfloat16):
    drawn = jax.random.normal(own_key, shape, jnp.float32) * deviation
    if len(cuts) > 0:
        drawn = shard_levels(own_key, shape, cuts, -0.22, 0.18) * drawn
    return jnp.clip(drawn, min=-limit, max=limit).astype(dtype)


def setup_inputs(seed: int = 0) -> dict:
    streams_of = jax.random.split(jax.random.key(seed), 14)
    return {
        "thickness": jnp.clip(jnp.exp(math.log(4.0) - 3.6927934 * jax.random.uniform(streams_of[0], (NCAT, NLAT, NLON), jnp.float32) ** shard_levels(streams_of[0], (NCAT, NLAT, NLON), ((0, 2), (1, 4), (2, 16)), -0.2, 0.2)), 0.099609375, 4.0).astype(jnp.bfloat16),
        "area": jnp.clip(jnp.exp(math.log(0.049804688) - 2.3038113 * jax.random.uniform(streams_of[1], (NCAT, NLAT, NLON), jnp.float32) ** shard_levels(streams_of[1], (NCAT, NLAT, NLON), ((0, 2), (1, 4), (2, 16)), -0.2, 0.2)), 0.0049743652, 0.049804688).astype(jnp.bfloat16),
        "ridge_weight": jnp.clip(jnp.exp(math.log(2.0) - 2.3025851 * jax.random.uniform(streams_of[2], (NCAT,), jnp.float32) ** shard_levels(streams_of[2], (NCAT,), ((0, 2),), -0.2, 0.2)), 0.2, 2.0),
        "cat_top": with_ends(jax.random.randint(streams_of[3], (NLAT, NLON), 1, NCAT + 1), jax.random.fold_in(streams_of[3], 1), 1, NCAT).astype(jnp.int32),
        "land_mask": with_ends((jax.random.randint(streams_of[4], (NLAT, NLON), 0, 10) < 9).astype(jnp.int32), jax.random.fold_in(streams_of[4], 1), 0, 1),
        "velocity_u": noise(streams_of[5], (NLAT, NLON), 0.3, 1.8, ((0, 4), (1, 16)), jnp.float32),
        "velocity_v": noise(streams_of[6], (NLAT, NLON), 0.3, 1.8, ((0, 4), (1, 16)), jnp.float32),
        "stress_div": noise(streams_of[7], (NLAT, NLON), 0.5, 3.0, ((0, 4), (1, 16)), jnp.float32),
        "stress_ten": noise(streams_of[8], (NLAT, NLON), 0.5, 3.0, ((0, 4), (1, 16)), jnp.float32),
        "stress_shear": noise(streams_of[9], (NLAT, NLON), 0.5, 3.0, ((0, 4), (1, 16)), jnp.float32),
        "wind_x": noise(streams_of[10], (NLAT, NLON), 1.0, 6.0, ((0, 4), (1, 16)), jnp.float32),
        "wind_y": noise(streams_of[11], (NLAT, NLON), 1.0, 6.0, ((0, 4), (1, 16)), jnp.float32),
        "water_drag": jnp.clip(jnp.exp(math.log(2.0) - 2.3025851 * jax.random.uniform(streams_of[12], (NLAT, NLON), jnp.float32) ** shard_levels(streams_of[12], (NLAT, NLON), ((0, 4), (1, 16)), -0.2, 0.2)), 0.2, 2.0),
    }


ELASTIC = 2.0
ECC_SQUARED = 4.0
DELTA_FLOOR = 0.05
CORIOLIS = 0.5

def slopes(along, across):
    return (0.5 * (along[:, :, 2:] - along[:, :, :-2]), 0.5 * (across[:, 2:, :] - across[:, :-2, :]))

def global_pad(along_stack, across_stack):
    along = jnp.pad(along_stack, ((0, 0), (0, 0), (1, 1)), mode='wrap')
    across = jnp.pad(across_stack, ((0, 0), (1, 1), (0, 0)))
    return (along, across)

def subcycle(velocity, stresses, statics):
    strength, mass, concentration, drag, push_x, push_y, wet = statics
    along, across = global_pad(velocity, velocity)
    ddx, ddy = slopes(along, across)
    divergence = ddx[0] + ddy[1]
    tension = ddx[0] - ddy[1]
    shearing = ddy[0] + ddx[1]
    delta = jnp.sqrt(divergence * divergence + (tension * tension + shearing * shearing) / ECC_SQUARED + DELTA_FLOOR * DELTA_FLOOR)
    relax = 1.0 / (1.0 + ELASTIC)
    viscous = ELASTIC * strength / delta
    first = wet * (stresses[0] + viscous * (divergence - delta)) * relax
    second = wet * (stresses[1] + viscous * tension / ECC_SQUARED) * relax
    cross = wet * (stresses[2] + viscous * shearing / ECC_SQUARED) * relax
    normal_x = 0.5 * (first + second)
    normal_y = 0.5 * (first - second)
    along_s, across_s = global_pad(jnp.stack([normal_x, cross]), jnp.stack([cross, normal_y]))
    sdx, sdy = slopes(along_s, across_s)
    force_x = sdx[0] + sdy[0]
    force_y = sdx[1] + sdy[1]
    denom = mass + drag + 1.0 - wet
    speed_u = wet * (mass * velocity[0] + force_x + concentration * push_x + CORIOLIS * mass * velocity[1]) / denom
    speed_v = wet * (mass * velocity[1] + force_y + concentration * push_y - CORIOLIS * mass * velocity[0]) / denom
    return (jnp.stack([speed_u, speed_v]), jnp.stack([first, second, cross]))

def reference(thickness, area, ridge_weight, cat_top, land_mask, velocity_u, velocity_v, stress_div, stress_ten, stress_shear, wind_x, wind_y, water_drag):

    def accumulate(level, carry):
        strength, mass, concentration = carry
        height = lax.dynamic_index_in_dim(thickness, level, 0, keepdims=False).astype(jnp.float32)
        present = (level < cat_top).astype(jnp.float32)
        cover = lax.dynamic_index_in_dim(area, level, 0, keepdims=False).astype(jnp.float32) * present
        weight = lax.dynamic_index_in_dim(ridge_weight, level, 0, keepdims=False)
        return (strength + weight * cover * height * height, mass + cover * height, concentration + cover)
    zeros = jnp.zeros(cat_top.shape, jnp.float32)
    strength, mass, concentration = lax.fori_loop(jnp.int32(0), jnp.int32(NCAT), accumulate, (zeros, zeros, zeros))
    wet = land_mask.astype(jnp.float32)
    statics = (strength, mass, concentration, water_drag, wind_x, wind_y, wet)
    velocity = jnp.stack([velocity_u, velocity_v])
    stresses = jnp.stack([stress_div, stress_ten, stress_shear])
    for step in range(SUB):
        velocity, stresses = subcycle(velocity, stresses, statics)
    return (velocity[0], velocity[1], stresses[0], stresses[1], stresses[2])
```

```python
import jax
import jax.numpy as jnp
from jax import lax
from jax.experimental import pallas as pl
from jax.experimental.pallas import tpu as pltpu
from jax.sharding import PartitionSpec as P

U, V, S1, S2, S12, WX, WY, DR, WT, ST, MA, CO = range(12)
NCAT = 20
ROWS = 256
COLS = 640
TILES = 5
CHUNKS = 15
AHEAD = 5
ORDER = (0, 4, 1, 2, 3)
TOP_ROW = 72
HEIGHT = 344
FIRST, LAST = 8, 41
LOADS = ((0, 16), (240, 16), (16, 48), (64, 64), (128, 64), (192, 48))
MESH = pl.DeviceIdType.MESH


def kernel(th, ar, weight, top, land, u0, v0, d0, t0, h0, wx0, wy0, dr0, out,
           F, T, A, TOP, LAND, PT, QT, LS, LR, XS, XR,
           cat_send, cat_recv, lon_send, lon_recv, edge_send, edge_recv, lat_send, lat_recv,
           load_sem, field_sem, out_sem):
    cat, lat, lon = lax.axis_index("cat"), lax.axis_index("lat"), lax.axis_index("lon")
    peer = (1 - cat, lat, lon)
    sides = ((cat, lat, lax.rem(lon + 15, 16)), (cat, lat, lax.rem(lon + 1, 16)))
    up = (cat, lax.rem(lat + 3, 4), lon)
    down = (cat, lax.rem(lat + 1, 4), lon)
    has_up, has_down = lat > 0, lat < 3

    barrier = pltpu.get_barrier_semaphore()
    for device in (peer, *sides, up, down):
        pl.semaphore_signal(barrier, inc=1, device_id=device, device_id_type=MESH)

    def load(i):
        start, size = LOADS[i]
        rows = pl.ds(start, size)
        return (
            pltpu.make_async_copy(top.at[rows, :], TOP.at[rows, :], load_sem.at[i, 0]),
            pltpu.make_async_copy(th.at[:, rows, :], T.at[:, rows, :], load_sem.at[i, 1]),
            pltpu.make_async_copy(ar.at[:, rows, :], A.at[:, rows, :], load_sem.at[i, 2]),
        )

    def field_loads():
        copies = [pltpu.make_async_copy(land, LAND, field_sem.at[8, 0])]
        for f, ref in enumerate((u0, v0, d0, t0, h0, wx0, wy0, dr0)):
            for j in range(TILES):
                copies.append(
                    pltpu.make_async_copy(
                        ref.at[:, pl.ds(j * 128, 128)], F.at[f, j, pl.ds(TOP_ROW, ROWS), :], field_sem.at[f, j]
                    )
                )
        return copies

    for i in range(3):
        for copy in load(i):
            copy.start()
    for copy in field_loads():
        copy.start()
    for i in range(3, len(LOADS)):
        for copy in load(i):
            copy.start()

    for f in range(5):
        for j in range(6):
            F[f, j, pl.ds(8 * FIRST - 8, 8), :] = jnp.zeros((8, 128), jnp.float32)
            F[f, j, pl.ds(8 * LAST + 8, 8), :] = jnp.zeros((8, 128), jnp.float32)

    @pl.when(lat == 0)
    def _():
        F[:, :, pl.ds(8 * FIRST, 8), :] = jnp.zeros((12, 6, 8, 128), jnp.float32)

    @pl.when(lat == 3)
    def _():
        F[:, :, pl.ds(8 * LAST, 8), :] = jnp.zeros((12, 6, 8, 128), jnp.float32)

    lane = lax.broadcasted_iota(jnp.int32, (8, 128), 1)
    lane16 = lax.broadcasted_iota(jnp.int32, (16, 128), 1)
    base = cat * NCAT

    def sums(block, carry):
        rows = pl.ds(pl.multiple_of(block * 16, 16), 16)
        for place, j in enumerate(ORDER):
            cols = pl.ds(j * 128, 128)
            limit = TOP[rows, cols] - base
            strength = jnp.zeros((16, 128), jnp.float32)
            mass = jnp.zeros((16, 128), jnp.float32)
            cover = jnp.zeros((16, 128), jnp.float32)
            for n in range(NCAT):
                h = T[n, rows, cols].astype(jnp.float32)
                c = A[n, rows, cols].astype(jnp.float32)
                c = jnp.where(limit > n, c, 0.0)
                m = c * h
                cover = cover + c
                mass = mass + m
                strength = strength + (weight[n] * h) * m
            PT[0, place, rows, :] = strength
            PT[1, place, rows, :] = mass
            PT[2, place, rows, :] = cover
        return carry

    def remote(src, dst, send, recv, device):
        return pltpu.make_async_remote_copy(
            src_ref=src, dst_ref=dst, send_sem=send, recv_sem=recv, device_id=device, device_id_type=MESH
        )

    def cat_message(tiles, rows, k):
        where = (slice(None), tiles, rows, slice(None))
        return remote(PT.at[where], QT.at[where], cat_send.at[k], cat_recv.at[k], peer)

    def border(c):
        return cat_message(pl.ds(0, 2), pl.ds(pl.multiple_of(8 + c * 16, 8), 16), c)

    def inner(c):
        return cat_message(pl.ds(2, 3), pl.ds(pl.multiple_of(8 + c * 16, 8), 16), CHUNKS + c)

    def edge(k):
        return cat_message(pl.ds(0, 5), pl.ds(248 * k, 8), 2 * CHUNKS + k)

    def lon_message(d, start, size, k):
        rows = pl.ds(start, size)
        return remote(XS.at[d, rows, :], XR.at[d, rows, :], lon_send.at[k, d], lon_recv.at[k, d], sides[d])

    def lon_chunk(d, c):
        return lon_message(d, pl.multiple_of(8 + c * 16, 8), 16, c)

    def lon_edge(d, k):
        return lon_message(d, 248 * k, 8, CHUNKS + k)

    def lon_static(d):
        return remote(LS.at[d], LR.at[d], edge_send.at[d], edge_recv.at[d], sides[d])

    def lat_message(d, k):
        fields = pl.ds(0, 9) if k == 0 else pl.ds(9, 3)
        here, there, device = ((FIRST + 1, LAST, up), (LAST - 1, FIRST, down))[d]
        return remote(
            F.at[fields, :, pl.ds(8 * here, 8), :], F.at[fields, :, pl.ds(8 * there, 8), :],
            lat_send.at[k, d], lat_recv.at[k, d], device,
        )

    def pack(first, count, send, row, size):
        iota = lane if size == 8 else lane16
        rows = pl.ds(row, size)
        from_rows = pl.ds(row + TOP_ROW, size)
        left = jnp.zeros((size, 128), jnp.float32)
        right = jnp.zeros((size, 128), jnp.float32)
        for i in range(count):
            mine = (iota >= 8 * i) & (iota < 8 * i + 8)
            a = F[first + i, 0, from_rows, :]
            b = F[first + i, 4, from_rows, :]
            left = jnp.where(mine, pltpu.roll(a, 8 * i, 1) if i else a, left)
            right = jnp.where(mine, pltpu.roll(b, 8 * i + 8, 1), right)
        send[0, rows, :] = left
        send[1, rows, :] = right

    def unpack(first, count, recv, row, size):
        iota = lane if size == 8 else lane16
        rows = pl.ds(row, size)
        a = recv[0, rows, :]
        b = recv[1, rows, :]
        for i in range(count):
            ahead = pltpu.roll(a, 128 - 8 * i, 1) if i else a
            behind = pltpu.roll(b, 120 - 8 * i, 1)
            F[first + i, 5, pl.ds(row + TOP_ROW, size), :] = jnp.where(
                iota < 8, ahead, jnp.where(iota >= 120, behind, 0.0)
            )

    def totals(places, row, size):
        for place in places:
            for f in range(3):
                F[ST + f, ORDER[place], pl.ds(row + TOP_ROW, size), :] = (
                    PT[f, place, pl.ds(row, size), :] + QT[f, place, pl.ds(row, size), :]
                )

    def right_less_left(before, here, after):
        ahead = pltpu.roll(jnp.where(lane == 0, after, here), 127, 1)
        behind = pltpu.roll(jnp.where(lane == 127, before, here), 1, 1)
        return ahead - behind

    def coefficients(band):
        rows = pl.ds(pl.multiple_of(8 * band, 8), 8)
        for j in range(6):
            wet = F[WT, j, rows, :]
            mass = F[MA, j, rows, :]
            cover = F[CO, j, rows, :]
            g = wet / (mass + F[DR, j, rows, :] + 1.0 - wet)
            push = g * cover
            F[MA, j, rows, :] = g * mass
            F[WX, j, rows, :] = push * F[WX, j, rows, :]
            F[WY, j, rows, :] = push * F[WY, j, rows, :]
            F[DR, j, rows, :] = 0.25 * g
            F[WT, j, rows, :] = wet * (1.0 / 3.0)

    def stress(band):
        row = pl.multiple_of(8 * band, 8)
        rows, above, below = pl.ds(row, 8), pl.ds(row - 1, 8), pl.ds(row + 1, 8)
        for j in range(6):
            before, after = (j + 5) % 6, (j + 1) % 6
            ux = right_less_left(F[U, before, rows, :], F[U, j, rows, :], F[U, after, rows, :])
            vx = right_less_left(F[V, before, rows, :], F[V, j, rows, :], F[V, after, rows, :])
            uy = F[U, j, below, :] - F[U, j, above, :]
            vy = F[V, j, below, :] - F[V, j, above, :]
            div, ten, shr = ux + vy, ux - vy, uy + vx
            square = 0.25 * (div * div + 0.25 * (ten * ten + shr * shr)) + 0.0025
            strength = F[ST, j, rows, :]
            half = strength * lax.rsqrt(square)
            eighth = 0.25 * half
            third = F[WT, j, rows, :]
            F[S1, j, rows, :] = third * (F[S1, j, rows, :] + half * div - 2.0 * strength)
            F[S2, j, rows, :] = third * (F[S2, j, rows, :] + eighth * ten)
            F[S12, j, rows, :] = third * (F[S12, j, rows, :] + eighth * shr)

    def momentum(band):
        row = pl.multiple_of(8 * band, 8)
        rows, above, below = pl.ds(row, 8), pl.ds(row - 1, 8), pl.ds(row + 1, 8)
        for j in range(6):
            around = ((j + 5) % 6, j, (j + 1) % 6)
            px = right_less_left(*(F[S1, k, rows, :] + F[S2, k, rows, :] for k in around))
            cx = right_less_left(*(F[S12, k, rows, :] for k in around))
            cy = F[S12, j, below, :] - F[S12, j, above, :]
            my = (F[S1, j, below, :] - F[S2, j, below, :]) - (F[S1, j, above, :] - F[S2, j, above, :])
            a, g = F[MA, j, rows, :], F[DR, j, rows, :]
            u, v = F[U, j, rows, :], F[V, j, rows, :]
            F[U, j, rows, :] = a * (u + 0.5 * v) + g * (px + 2.0 * cy) + F[WX, j, rows, :]
            F[V, j, rows, :] = a * (v - 0.5 * u) + g * (2.0 * cx + my) + F[WY, j, rows, :]

    def step(t):
        @pl.when(t <= LAST - FIRST)
        def _():
            coefficients(t + FIRST)
            stress(t + FIRST)

        for lag in range(1, 8):
            @pl.when((t >= lag) & (t <= LAST - FIRST + lag))
            def _():
                (momentum if lag % 2 else stress)(t + (FIRST - lag))

    def out_copies(row, size, k):
        return [
            pltpu.make_async_copy(
                F.at[pl.ds(0, 5), j, pl.ds(row + TOP_ROW, size), :],
                out.at[:, pl.ds(row, size), pl.ds(j * 128, 128)],
                out_sem.at[k, j],
            )
            for j in range(TILES)
        ]

    for i, block in ((0, 0), (1, 15)):
        for copy in load(i):
            copy.wait()
        sums(block, 0)
    pl.semaphore_wait(barrier, 5)
    edge(0).start()
    edge(1).start()
    for copy in load(2):
        copy.wait()
    lax.fori_loop(1, 4, sums, 0)
    border(0).start()
    border(1).start()
    inner(0).start()
    border(2).start()
    inner(1).start()

    for copy in field_loads():
        copy.wait()

    def given(block, carry):
        row = pl.multiple_of(block * 16, 16)
        for j in range(TILES):
            F[WT, j, pl.ds(row + TOP_ROW, 16), :] = LAND[pl.ds(row, 16), pl.ds(j * 128, 128)].astype(jnp.float32)
        pack(0, 9, LS, row, 16)
        return carry

    lax.fori_loop(0, 16, given, 0)
    for d in range(2):
        lon_static(d).start()

    for copy in load(3):
        copy.wait()
    lax.fori_loop(4, 8, sums, 0)
    border(3).start()
    inner(2).start()

    for k in range(2):
        edge(k).wait_recv()
        totals(range(5), 248 * k, 8)
        pack(ST, 3, XS, 248 * k, 8)
        for d in range(2):
            lon_edge(d, k).start()
    for i in (4, 5):
        for copy in load(i):
            copy.wait()
    lax.fori_loop(8, 15, sums, 0)

    for d in range(2):
        lon_static(d).wait_recv()

    def take(block, carry):
        unpack(0, 9, LR, pl.multiple_of(block * 16, 16), 16)
        return carry

    lax.fori_loop(0, 16, take, 0)
    for k in range(2):
        for d in range(2):
            lon_edge(d, k).wait_recv()
        unpack(ST, 3, XR, 248 * k, 8)

    @pl.when(has_up)
    def _():
        lat_message(0, 0).start()
        lat_message(0, 1).start()

    @pl.when(has_down)
    def _():
        lat_message(1, 0).start()
        lat_message(1, 1).start()

    for c in range(4, AHEAD + 1):
        border(c).start()
        inner(c - 1).start()

    def columns(c):
        row = pl.multiple_of(8 + c * 16, 8)
        border(c).wait_recv()
        totals(range(2), row, 16)
        pack(ST, 3, XS, row, 16)
        for d in range(2):
            lon_chunk(d, c).start()

    columns(0)

    @pl.when(has_down)
    def _():
        lat_message(0, 0).wait_recv()
        lat_message(0, 1).wait_recv()

    @pl.when(has_up)
    def _():
        lat_message(1, 0).wait_recv()
        lat_message(1, 1).wait_recv()

    @pl.when(has_up)
    def _():
        lat_message(0, 0).wait_send()
        lat_message(0, 1).wait_send()

    @pl.when(has_down)
    def _():
        lat_message(1, 0).wait_send()
        lat_message(1, 1).wait_send()

    def early(t, carry):
        step(t)
        return carry

    lax.fori_loop(0, 2, early, 0)

    def chunk(c, carry):
        @pl.when(c < CHUNKS - 1)
        def _():
            columns(c + 1)

        row = pl.multiple_of(8 + c * 16, 8)
        for d in range(2):
            lon_chunk(d, c).wait_recv()
        unpack(ST, 3, XR, row, 16)
        inner(c).wait_recv()

        @pl.when(c + AHEAD + 1 < CHUNKS)
        def _():
            border(c + AHEAD + 1).start()

        @pl.when(c + AHEAD < CHUNKS)
        def _():
            inner(c + AHEAD).start()

        totals(range(2, 5), row, 16)
        lax.fori_loop(2 * c + 2, 2 * c + 4, early, 0)

        @pl.when(c >= 3)
        def _():
            for copy in out_copies(pl.multiple_of((c - 3) * 16, 16), 16, c - 3):
                copy.start()

        return carry

    lax.fori_loop(0, CHUNKS, chunk, 0)
    lax.fori_loop(32, 40, early, 0)
    last = CHUNKS - 3
    for copy in out_copies(last * 16, ROWS - last * 16, last):
        copy.start()

    def finish(c, carry):
        border(c).wait_send()
        inner(c).wait_send()
        for d in range(2):
            lon_chunk(d, c).wait_send()

        @pl.when(c < last)
        def _():
            for copy in out_copies(pl.multiple_of(c * 16, 16), 16, c):
                copy.wait()

        return carry

    lax.fori_loop(0, CHUNKS, finish, 0)
    for k in range(2):
        edge(k).wait_send()
        lon_static(k).wait_send()
        for d in range(2):
            lon_edge(d, k).wait_send()
    for copy in out_copies(last * 16, ROWS - last * 16, last):
        copy.wait()


def shards(*arrays):
    dma = pltpu.SemaphoreType.DMA
    f32 = jnp.float32
    hbm = pl.BlockSpec(memory_space=pl.ANY)
    specs = [hbm] * len(arrays)
    specs[2] = pl.BlockSpec(memory_space=pltpu.SMEM)
    result = pl.pallas_call(
        kernel,
        out_shape=jax.ShapeDtypeStruct((5, ROWS, COLS), f32),
        in_specs=specs,
        out_specs=pl.BlockSpec(memory_space=pl.ANY),
        scratch_shapes=[
            pltpu.VMEM((12, 6, HEIGHT, 128), f32),
            pltpu.VMEM((NCAT, ROWS, COLS), jnp.bfloat16),
            pltpu.VMEM((NCAT, ROWS, COLS), jnp.bfloat16),
            pltpu.VMEM((ROWS, COLS), jnp.int32),
            pltpu.VMEM((ROWS, COLS), jnp.int32),
            pltpu.VMEM((3, TILES, ROWS, 128), f32),
            pltpu.VMEM((3, TILES, ROWS, 128), f32),
            pltpu.VMEM((2, ROWS, 128), f32),
            pltpu.VMEM((2, ROWS, 128), f32),
            pltpu.VMEM((2, ROWS, 128), f32),
            pltpu.VMEM((2, ROWS, 128), f32),
            dma((2 * CHUNKS + 2,)),
            dma((2 * CHUNKS + 2,)),
            dma((CHUNKS + 2, 2)),
            dma((CHUNKS + 2, 2)),
            dma((2,)),
            dma((2,)),
            dma((2, 2)),
            dma((2, 2)),
            dma((len(LOADS), 3)),
            dma((9, TILES)),
            dma((CHUNKS, TILES)),
        ],
        compiler_params=pltpu.CompilerParams(
            collective_id=0, has_side_effects=True, vmem_limit_bytes=60 * 2**20 + 2**18
        ),
        name="ice",
    )(*arrays)
    return tuple(result[i] for i in range(5))


def solution(mesh):
    block = P("cat", "lat", "lon")
    plane = P("lat", "lon")
    return jax.shard_map(
        shards,
        mesh=mesh,
        in_specs=(block, block, P("cat"), *[plane] * 10),
        out_specs=(plane,) * 5,
        check_vma=False,
    )
```

```python
import jax
import jax.numpy as jnp
from jax import lax
from jax.experimental import pallas as pl
from jax.experimental.pallas import tpu as pltpu
from jax.sharding import PartitionSpec as P

U, V, S1, S2, S12, WX, WY, DR, WT, ST, MA, CO = range(12)
NCAT = 20
ROWS = 256
COLS = 640
TILES = 5
CHUNKS = 15
COLUMNS_AHEAD = 3
BORDERS_AHEAD = 8
INNERS_AHEAD = 6
ORDER = (0, 4, 1, 2, 3)
TOP_ROW = 72
HEIGHT = 344
FIRST, LAST = 8, 41
LOADS = ((0, 16), (240, 16), (16, 48), (64, 64), (128, 64), (192, 48))
MESH = pl.DeviceIdType.MESH


def kernel(th, ar, weight, top, land, u0, v0, d0, t0, h0, wx0, wy0, dr0, out,
           F, W, T, A, TOP, LAND, PT, QT, LS, LR, XS, XR,
           cat_send, cat_recv, lon_send, lon_recv, edge_send, edge_recv, lat_send, lat_recv,
           load_sem, field_sem):
    cat, lat, lon = lax.axis_index("cat"), lax.axis_index("lat"), lax.axis_index("lon")
    peer = (1 - cat, lat, lon)
    sides = ((cat, lat, lax.rem(lon + 15, 16)), (cat, lat, lax.rem(lon + 1, 16)))
    up = (cat, lax.rem(lat + 3, 4), lon)
    down = (cat, lax.rem(lat + 1, 4), lon)
    has_up, has_down = lat > 0, lat < 3

    def load(i):
        start, size = LOADS[i]
        rows = pl.ds(start, size)
        return (
            pltpu.make_async_copy(top.at[rows, :], TOP.at[rows, :], load_sem.at[i, 0]),
            pltpu.make_async_copy(th.at[:, rows, :], T.at[:, rows, :], load_sem.at[i, 1]),
            pltpu.make_async_copy(ar.at[:, rows, :], A.at[:, rows, :], load_sem.at[i, 2]),
        )

    def field_loads():
        copies = [pltpu.make_async_copy(land, LAND, field_sem.at[8, 0])]
        for f, ref in enumerate((u0, v0, d0, t0, h0, wx0, wy0, dr0)):
            for j in range(TILES):
                copies.append(
                    pltpu.make_async_copy(
                        ref.at[:, pl.ds(j * 128, 128)], F.at[f, j, pl.ds(TOP_ROW, ROWS), :], field_sem.at[f, j]
                    )
                )
        return copies

    weights = pltpu.make_async_copy(weight, W, field_sem.at[8, 1])
    for i in range(2):
        for copy in load(i):
            copy.start()
    weights.start()
    barrier = pltpu.get_barrier_semaphore()
    for device in (peer, *sides, up, down):
        pl.semaphore_signal(barrier, inc=1, device_id=device, device_id_type=MESH)
    for copy in load(2):
        copy.start()

    @pl.when(lat == 0)
    def _():
        F[:, :, pl.ds(8 * FIRST, 8), :] = jnp.zeros((12, 6, 8, 128), jnp.float32)

    @pl.when(lat == 3)
    def _():
        F[:, :, pl.ds(8 * LAST, 8), :] = jnp.zeros((12, 6, 8, 128), jnp.float32)

    lane = lax.broadcasted_iota(jnp.int32, (8, 128), 1)
    lane16 = lax.broadcasted_iota(jnp.int32, (16, 128), 1)
    base = cat * NCAT

    def sums(block, carry):
        rows = pl.ds(pl.multiple_of(block * 16, 16), 16)
        for place, j in enumerate(ORDER):
            cols = pl.ds(j * 128, 128)
            limit = TOP[rows, cols] - base
            strength = jnp.zeros((16, 128), jnp.float32)
            mass = jnp.zeros((16, 128), jnp.float32)
            cover = jnp.zeros((16, 128), jnp.float32)
            for n in range(NCAT):
                h = T[n, rows, cols].astype(jnp.float32)
                c = A[n, rows, cols].astype(jnp.float32)
                c = jnp.where(limit > n, c, 0.0)
                m = c * h
                cover = cover + c
                mass = mass + m
                strength = strength + (W[n] * h) * m
            PT[0, place, rows, :] = strength
            PT[1, place, rows, :] = mass
            PT[2, place, rows, :] = cover
        return carry

    def remote(src, dst, send, recv, device):
        return pltpu.make_async_remote_copy(
            src_ref=src, dst_ref=dst, send_sem=send, recv_sem=recv, device_id=device, device_id_type=MESH
        )

    def cat_message(tiles, rows, k):
        where = (slice(None), tiles, rows, slice(None))
        return remote(PT.at[where], QT.at[where], cat_send.at[k], cat_recv.at[k], peer)

    def border(c):
        return cat_message(pl.ds(0, 2), pl.ds(pl.multiple_of(8 + c * 16, 8), 16), c)

    def inner(c):
        return cat_message(pl.ds(2, 3), pl.ds(pl.multiple_of(8 + c * 16, 8), 16), CHUNKS + c)

    def edge(k):
        return cat_message(pl.ds(0, 5), pl.ds(248 * k, 8), 2 * CHUNKS + k)

    def lon_message(d, start, size, k):
        rows = pl.ds(start, size)
        return remote(XS.at[d, rows, :], XR.at[d, rows, :], lon_send.at[k, d], lon_recv.at[k, d], sides[d])

    def lon_chunk(d, c):
        return lon_message(d, pl.multiple_of(8 + c * 16, 8), 16, c)

    def lon_edge(d, k):
        return lon_message(d, 248 * k, 8, CHUNKS + k)

    def lon_static(d):
        return remote(LS.at[d], LR.at[d], edge_send.at[d], edge_recv.at[d], sides[d])

    def lat_message(d, k):
        fields, tiles = (
            (pl.ds(0, 9), pl.ds(0, TILES)), (pl.ds(9, 3), pl.ds(0, TILES)), (pl.ds(0, 12), pl.ds(TILES, 1))
        )[k]
        here, there, device = ((FIRST + 1, LAST, up), (LAST - 1, FIRST, down))[d]
        return remote(
            F.at[fields, tiles, pl.ds(8 * here, 8), :], F.at[fields, tiles, pl.ds(8 * there, 8), :],
            lat_send.at[k, d], lat_recv.at[k, d], device,
        )

    def pack(first, count, send, row, size):
        iota = lane if size == 8 else lane16
        rows = pl.ds(row, size)
        from_rows = pl.ds(row + TOP_ROW, size)
        left = jnp.zeros((size, 128), jnp.float32)
        right = jnp.zeros((size, 128), jnp.float32)
        for i in range(count):
            mine = (iota >= 8 * i) & (iota < 8 * i + 8)
            a = F[first + i, 0, from_rows, :]
            b = F[first + i, 4, from_rows, :]
            left = jnp.where(mine, pltpu.roll(a, 8 * i, 1) if i else a, left)
            right = jnp.where(mine, pltpu.roll(b, 8 * i + 8, 1), right)
        send[0, rows, :] = left
        send[1, rows, :] = right

    def unpack(first, count, recv, row, size):
        iota = lane if size == 8 else lane16
        rows = pl.ds(row, size)
        a = recv[0, rows, :]
        b = recv[1, rows, :]
        for i in range(count):
            ahead = pltpu.roll(a, 128 - 8 * i, 1) if i else a
            behind = pltpu.roll(b, 120 - 8 * i, 1)
            F[first + i, 5, pl.ds(row + TOP_ROW, size), :] = jnp.where(
                iota < 8, ahead, jnp.where(iota >= 120, behind, 0.0)
            )

    def totals(places, row, size):
        for place in places:
            for f in range(3):
                F[ST + f, ORDER[place], pl.ds(row + TOP_ROW, size), :] = (
                    PT[f, place, pl.ds(row, size), :] + QT[f, place, pl.ds(row, size), :]
                )

    def right_less_left(before, here, after):
        ahead = pltpu.roll(jnp.where(lane == 0, after, here), 127, 1)
        behind = pltpu.roll(jnp.where(lane == 127, before, here), 1, 1)
        return ahead - behind

    def coefficients(band):
        rows = pl.ds(pl.multiple_of(8 * band, 8), 8)
        for j in range(6):
            wet = F[WT, j, rows, :]
            mass = F[MA, j, rows, :]
            cover = F[CO, j, rows, :]
            g = wet / (mass + F[DR, j, rows, :] + 1.0 - wet)
            push = g * cover
            F[MA, j, rows, :] = g * mass
            F[WX, j, rows, :] = push * F[WX, j, rows, :]
            F[WY, j, rows, :] = push * F[WY, j, rows, :]
            F[DR, j, rows, :] = 0.25 * g
            F[WT, j, rows, :] = wet * (1.0 / 3.0)

    def stress(band, last=None):
        row = pl.multiple_of(8 * band, 8)
        rows, above, below = pl.ds(row, 8), pl.ds(row - 1, 8), pl.ds(row + 1, 8)
        for j in range(6):
            before, after = (j + 5) % 6, (j + 1) % 6
            ux = right_less_left(F[U, before, rows, :], F[U, j, rows, :], F[U, after, rows, :])
            vx = right_less_left(F[V, before, rows, :], F[V, j, rows, :], F[V, after, rows, :])
            uy = F[U, j, below, :] - F[U, j, above, :]
            vy = F[V, j, below, :] - F[V, j, above, :]
            div, ten, shr = ux + vy, ux - vy, uy + vx
            square = 0.25 * (div * div + 0.25 * (ten * ten + shr * shr)) + 0.0025
            strength = F[ST, j, rows, :]
            half = strength * lax.rsqrt(square)
            eighth = 0.25 * half
            third = F[WT, j, rows, :]
            s1 = third * (F[S1, j, rows, :] + half * div - 2.0 * strength)
            s2 = third * (F[S2, j, rows, :] + eighth * ten)
            s12 = third * (F[S12, j, rows, :] + eighth * shr)
            F[S1, j, rows, :] = s1
            F[S2, j, rows, :] = s2
            F[S12, j, rows, :] = s12
            if last is not None and j < TILES:
                place = (pl.ds(last, 8), pl.ds(j * 128, 128))
                out[(S1, *place)] = s1
                out[(S2, *place)] = s2
                out[(S12, *place)] = s12

    def momentum(band, last=None):
        row = pl.multiple_of(8 * band, 8)
        rows, above, below = pl.ds(row, 8), pl.ds(row - 1, 8), pl.ds(row + 1, 8)
        for j in range(6):
            around = ((j + 5) % 6, j, (j + 1) % 6)
            px = right_less_left(*(F[S1, k, rows, :] + F[S2, k, rows, :] for k in around))
            cx = right_less_left(*(F[S12, k, rows, :] for k in around))
            cy = F[S12, j, below, :] - F[S12, j, above, :]
            my = (F[S1, j, below, :] - F[S2, j, below, :]) - (F[S1, j, above, :] - F[S2, j, above, :])
            a, g = F[MA, j, rows, :], F[DR, j, rows, :]
            u, v = F[U, j, rows, :], F[V, j, rows, :]
            next_u = a * (u + 0.5 * v) + g * (px + 2.0 * cy) + F[WX, j, rows, :]
            next_v = a * (v - 0.5 * u) + g * (2.0 * cx + my) + F[WY, j, rows, :]
            if last is None:
                F[U, j, rows, :] = next_u
                F[V, j, rows, :] = next_v
            elif j < TILES:
                place = (pl.ds(last, 8), pl.ds(j * 128, 128))
                out[(U, *place)] = next_u
                out[(V, *place)] = next_v

    def half_stage(lag, band):
        last = None
        if lag >= 6:
            row = 8 * (band - FIRST - 1)
            last = max(row, 0) if isinstance(band, int) else pl.multiple_of(jnp.maximum(row, 0), 8)
            if isinstance(band, int) and band == LAST:
                last = None
        (momentum if lag % 2 else stress)(band, last)

    def step(t, carry):
        coefficients(t + FIRST)
        for lag in range(8):
            half_stage(lag, t + (FIRST - lag))
        return carry

    weights.wait()
    for i, block in ((0, 0), (1, 15)):
        for copy in load(i):
            copy.wait()
        if i == 1:
            for copy in field_loads():
                copy.start()
            for late in range(3, len(LOADS)):
                for copy in load(late):
                    copy.start()
        sums(block, 0)
        if i == 0:
            pl.semaphore_wait(barrier, 5)
        edge(i).start()
    for copy in load(2):
        copy.wait()
    lax.fori_loop(1, 4, sums, 0)
    for c in range(3):
        border(c).start()
    inner(0).start()

    for copy in field_loads():
        copy.wait()

    def given(block, carry):
        row = pl.multiple_of(block * 16, 16)
        for j in range(TILES):
            F[WT, j, pl.ds(row + TOP_ROW, 16), :] = LAND[pl.ds(row, 16), pl.ds(j * 128, 128)].astype(jnp.float32)
        pack(0, 9, LS, row, 16)
        return carry

    lax.fori_loop(0, 16, given, 0)
    for d in range(2):
        lon_static(d).start()

    def to_rows(k):
        @pl.when(has_up)
        def _():
            lat_message(0, k).start()

        @pl.when(has_down)
        def _():
            lat_message(1, k).start()

    to_rows(0)
    for copy in load(3):
        copy.wait()
    lax.fori_loop(4, 8, sums, 0)
    border(3).start()
    inner(1).start()
    border(4).start()

    for k in range(2):
        edge(k).wait_recv()
        totals(range(5), 248 * k, 8)
        pack(ST, 3, XS, 248 * k, 8)
        for d in range(2):
            lon_edge(d, k).start()
    to_rows(1)
    for i in (4, 5):
        for copy in load(i):
            copy.wait()
    lax.fori_loop(8, 15, sums, 0)

    for d in range(2):
        lon_static(d).wait_recv()

    def take(block, carry):
        unpack(0, 9, LR, pl.multiple_of(block * 16, 16), 16)
        return carry

    lax.fori_loop(0, 16, take, 0)
    for k in range(2):
        for d in range(2):
            lon_edge(d, k).wait_recv()
        unpack(ST, 3, XR, 248 * k, 8)
    to_rows(2)
    for c in range(5, BORDERS_AHEAD):
        inner(c - 3).start()
        border(c).start()
    inner(BORDERS_AHEAD - 3).start()

    def columns(c):
        row = pl.multiple_of(8 + c * 16, 8)
        border(c).wait_recv()
        totals(range(2), row, 16)
        pack(ST, 3, XS, row, 16)
        for d in range(2):
            lon_chunk(d, c).start()

    for c in range(COLUMNS_AHEAD):
        columns(c)

    @pl.when(has_down)
    def _():
        for k in range(3):
            lat_message(0, k).wait_recv()
            lat_message(1, k).wait_send()

    @pl.when(has_up)
    def _():
        for k in range(3):
            lat_message(1, k).wait_recv()
            lat_message(0, k).wait_send()

    lax.fori_loop(0, 2, step, 0)

    def chunk(c, carry):
        @pl.when(c + COLUMNS_AHEAD < CHUNKS)
        def _():
            columns(c + COLUMNS_AHEAD)

        row = pl.multiple_of(8 + c * 16, 8)
        for d in range(2):
            lon_chunk(d, c).wait_recv()
        unpack(ST, 3, XR, row, 16)
        inner(c).wait_recv()

        @pl.when(c + BORDERS_AHEAD < CHUNKS)
        def _():
            border(c + BORDERS_AHEAD).start()

        @pl.when(c + INNERS_AHEAD < CHUNKS)
        def _():
            inner(c + INNERS_AHEAD).start()

        totals(range(2, 5), row, 16)
        lax.fori_loop(2 * c + 2, 2 * c + 4, step, 0)
        return carry

    lax.fori_loop(0, CHUNKS, chunk, 0)
    lax.fori_loop(32, 34, step, 0)
    for t in range(34, 40):
        for lag in range(t - 33, 8):
            half_stage(lag, t + FIRST - lag)

    def finish(c, carry):
        border(c).wait_send()
        inner(c).wait_send()
        for d in range(2):
            lon_chunk(d, c).wait_send()
        return carry

    lax.fori_loop(0, CHUNKS, finish, 0)
    for k in range(2):
        edge(k).wait_send()
        lon_static(k).wait_send()
        for d in range(2):
            lon_edge(d, k).wait_send()


def shards(*arrays):
    dma = pltpu.SemaphoreType.DMA
    f32 = jnp.float32
    result = pl.pallas_call(
        kernel,
        out_shape=jax.ShapeDtypeStruct((5, ROWS, COLS), f32),
        in_specs=[pl.BlockSpec(memory_space=pltpu.HBM)] * len(arrays),
        out_specs=pl.BlockSpec(memory_space=pltpu.VMEM),
        scratch_shapes=[
            pltpu.VMEM((12, 6, HEIGHT, 128), f32),
            pltpu.SMEM((NCAT,), f32),
            pltpu.VMEM((NCAT, ROWS, COLS), jnp.bfloat16),
            pltpu.VMEM((NCAT, ROWS, COLS), jnp.bfloat16),
            pltpu.VMEM((ROWS, COLS), jnp.int32),
            pltpu.VMEM((ROWS, COLS), jnp.int32),
            pltpu.VMEM((3, TILES, ROWS, 128), f32),
            pltpu.VMEM((3, TILES, ROWS, 128), f32),
            pltpu.VMEM((2, ROWS, 128), f32),
            pltpu.VMEM((2, ROWS, 128), f32),
            pltpu.VMEM((2, ROWS, 128), f32),
            pltpu.VMEM((2, ROWS, 128), f32),
            dma((2 * CHUNKS + 2,)),
            dma((2 * CHUNKS + 2,)),
            dma((CHUNKS + 2, 2)),
            dma((CHUNKS + 2, 2)),
            dma((2,)),
            dma((2,)),
            dma((3, 2)),
            dma((3, 2)),
            dma((len(LOADS), 3)),
            dma((9, TILES)),
        ],
        compiler_params=pltpu.CompilerParams(
            collective_id=0, has_side_effects=True, vmem_limit_bytes=44 * 2**20
        ),
        name="ice",
    )(*(pltpu.with_memory_space_constraint(a, pltpu.HBM) for a in arrays))
    return tuple(result[i] for i in range(5))


def solution(mesh):
    block = P("cat", "lat", "lon")
    plane = P("lat", "lon")
    return jax.shard_map(
        shards,
        mesh=mesh,
        in_specs=(block, block, P("cat"), *[plane] * 10),
        out_specs=(plane,) * 5,
        check_vma=False,
    )
```

```python
import jax
import jax.numpy as jnp
from jax import lax
from jax.experimental import pallas as pl
from jax.experimental.pallas import tpu as pltpu
from jax.sharding import PartitionSpec as P

U, V, S1, S2, S12, WX, WY, DR, WT, ST, MA, CO = range(12)
NCAT = 20
ROWS = 256
COLS = 640
TILES = 5
CHUNKS = 15
COLUMNS_AHEAD = 6
BORDERS_AHEAD = 12
INNERS_AHEAD = 6
ORDER = (0, 4, 1, 2, 3)
TOP_ROW = 72
HEIGHT = 344
FIRST, LAST = 8, 41
LOADS = ((0, 16), (240, 16), (16, 48), (64, 64), (128, 64), (192, 48))
TOPS = ((0, 16), (240, 16), (16, 224))
MESH = pl.DeviceIdType.MESH


def kernel(th, ar, weight, top, land, u0, v0, d0, t0, h0, wx0, wy0, dr0, out,
           F, W, TA, TOP, LAND, PT, QT, LS, LR, XS, XR,
           cat_send, cat_recv, lon_send, lon_recv, edge_send, edge_recv, lat_send, lat_recv,
           load_sem, top_sem, field_sem, near):
    cat, lat, lon = lax.axis_index("cat"), lax.axis_index("lat"), lax.axis_index("lon")
    peer = (1 - cat, lat, lon)
    sides = ((cat, lat, lax.rem(lon + 15, 16)), (cat, lat, lax.rem(lon + 1, 16)))
    up = (cat, lax.rem(lat + 3, 4), lon)
    down = (cat, lax.rem(lat + 1, 4), lon)
    has_up, has_down = lat > 0, lat < 3

    even = lax.rem(lon, 2) == 0

    def load_rows(i):
        return pl.ds(*LOADS[i])

    def start_load(i):
        rows = load_rows(i)
        if i < len(TOPS):
            some = pl.ds(*TOPS[i])
            pltpu.make_async_copy(top.at[some, :], TOP.at[some, :], top_sem.at[i]).start()
        for k, ref in enumerate((th, ar)):
            pltpu.make_async_copy(ref.at[:, rows, :], TA.at[k, :, rows, :], load_sem.at[i]).start()

    def wait_load(i):
        if i < len(TOPS):
            some = TOP.at[pl.ds(*TOPS[i]), :]
            pltpu.make_async_copy(some, some, top_sem.at[i]).wait()
        both = TA.at[:, :, load_rows(i), :]
        pltpu.make_async_copy(both, both, load_sem.at[i]).wait()

    lands = pltpu.make_async_copy(land, LAND, field_sem.at[1])
    weights = pltpu.make_async_copy(weight, W, field_sem.at[2])

    def start_fields():
        for f, ref in enumerate((u0, v0, d0, t0, h0, wx0, wy0, dr0)):
            for j in range(TILES):
                pltpu.make_async_copy(
                    ref.at[:, pl.ds(j * 128, 128)], F.at[f, j, pl.ds(TOP_ROW, ROWS), :], field_sem.at[0]
                ).start()
        lands.start()

    def wait_fields():
        given = F.at[pl.ds(0, 8), pl.ds(0, TILES), pl.ds(TOP_ROW, ROWS), :]
        pltpu.make_async_copy(given, given, field_sem.at[0]).wait()
        lands.wait()

    start_load(0)
    weights.start()
    start_load(1)
    barrier = pltpu.get_barrier_semaphore()
    for device in (peer, up, down):
        pl.semaphore_signal(barrier, inc=1, device_id=device, device_id_type=MESH)

    @pl.when(even)
    def _():
        for device in sides:
            pl.semaphore_signal(barrier, inc=1, device_id=device, device_id_type=MESH)

    def enter():
        @pl.when(even)
        def _():
            pl.semaphore_wait(barrier, 3)

        @pl.when(jnp.logical_not(even))
        def _():
            pl.semaphore_wait(barrier, 5)
            for device in sides:
                pl.semaphore_signal(near, inc=1, device_id=device, device_id_type=MESH)

    start_load(2)
    start_load(3)

    @pl.when(lat == 0)
    def _():
        F[:, :, pl.ds(8 * FIRST, 8), :] = jnp.zeros((12, 6, 8, 128), jnp.float32)

    @pl.when(lat == 3)
    def _():
        F[:, :, pl.ds(8 * LAST, 8), :] = jnp.zeros((12, 6, 8, 128), jnp.float32)

    lane = lax.broadcasted_iota(jnp.int32, (8, 128), 1)
    lane16 = lax.broadcasted_iota(jnp.int32, (16, 128), 1)
    base = cat * NCAT

    def sums(block, carry):
        rows = pl.ds(pl.multiple_of(block * 16, 16), 16)
        for place, j in enumerate(ORDER):
            cols = pl.ds(j * 128, 128)
            limit = TOP[rows, cols] - base
            strength = jnp.zeros((16, 128), jnp.float32)
            mass = jnp.zeros((16, 128), jnp.float32)
            cover = jnp.zeros((16, 128), jnp.float32)
            for n in range(NCAT):
                h = TA[0, n, rows, cols].astype(jnp.float32)
                c = TA[1, n, rows, cols].astype(jnp.float32)
                c = jnp.where(limit > n, c, 0.0)
                m = c * h
                cover = cover + c
                mass = mass + m
                strength = strength + (W[n] * h) * m
            PT[0, place, rows, :] = strength
            PT[1, place, rows, :] = mass
            PT[2, place, rows, :] = cover
        return carry

    def remote(src, dst, send, recv, device):
        return pltpu.make_async_remote_copy(
            src_ref=src, dst_ref=dst, send_sem=send, recv_sem=recv, device_id=device, device_id_type=MESH
        )

    def cat_message(tiles, rows, k):
        where = (slice(None), tiles, rows, slice(None))
        return remote(PT.at[where], QT.at[where], cat_send, cat_recv.at[k], peer)

    def border(c):
        return cat_message(pl.ds(0, 2), pl.ds(pl.multiple_of(8 + c * 16, 8), 16), c)

    def inner(c):
        return cat_message(pl.ds(2, 3), pl.ds(pl.multiple_of(8 + c * 16, 8), 16), CHUNKS + c)

    def last_inner(k):
        return cat_message(pl.ds(2, 3), pl.ds(ROWS - 24 + 8 * k, 8), 2 * CHUNKS - 1 + k)

    def edge(k):
        return cat_message(pl.ds(0, 5), pl.ds(248 * k, 8), 2 * CHUNKS + 1 + k)

    def start_columns(start, size, k):
        rows = pl.ds(start, size)
        for d in range(2):
            remote(XS.at[d, rows, :], XR.at[d, rows, :], lon_send, lon_recv.at[k], sides[d]).start()

    def wait_columns(start, size, k):
        rows = pl.ds(start, size)
        remote(XS.at[:, rows, :], XR.at[:, rows, :], lon_send, lon_recv.at[k], sides[0]).wait_recv()

    def lat_message(d, k):
        fields, tiles = (
            (pl.ds(0, 9), pl.ds(0, TILES)), (pl.ds(9, 3), pl.ds(0, TILES)), (pl.ds(0, 12), pl.ds(TILES, 1))
        )[k]
        return lat_copy(d, fields, tiles)

    def lat_copy(d, fields, tiles):
        here, there, device = ((FIRST + 1, LAST, up), (LAST - 1, FIRST, down))[d]
        return remote(
            F.at[fields, tiles, pl.ds(8 * here, 8), :], F.at[fields, tiles, pl.ds(8 * there, 8), :],
            lat_send.at[d], lat_recv.at[d], device,
        )

    def pack(first, count, send, row, size):
        iota = lane if size == 8 else lane16
        rows = pl.ds(row, size)
        from_rows = pl.ds(row + TOP_ROW, size)
        left = jnp.zeros((size, 128), jnp.float32)
        right = jnp.zeros((size, 128), jnp.float32)
        for i in range(count):
            mine = (iota >= 8 * i) & (iota < 8 * i + 8)
            a = F[first + i, 0, from_rows, :]
            b = F[first + i, 4, from_rows, :]
            left = jnp.where(mine, pltpu.roll(a, 8 * i, 1) if i else a, left)
            right = jnp.where(mine, pltpu.roll(b, 8 * i + 8, 1), right)
        send[0, rows, :] = left
        send[1, rows, :] = right

    def unpack(first, count, recv, row, size):
        iota = lane if size == 8 else lane16
        rows = pl.ds(row, size)
        a = recv[0, rows, :]
        b = recv[1, rows, :]
        for i in range(count):
            ahead = pltpu.roll(a, 128 - 8 * i, 1) if i else a
            behind = pltpu.roll(b, 120 - 8 * i, 1)
            F[first + i, 5, pl.ds(row + TOP_ROW, size), :] = jnp.where(
                iota < 8, ahead, jnp.where(iota >= 120, behind, 0.0)
            )

    def totals(places, row, size):
        for place in places:
            for f in range(3):
                F[ST + f, ORDER[place], pl.ds(row + TOP_ROW, size), :] = (
                    PT[f, place, pl.ds(row, size), :] + QT[f, place, pl.ds(row, size), :]
                )

    def right_less_left(before, here, after):
        ahead = pltpu.roll(jnp.where(lane == 0, after, here), 127, 1)
        behind = pltpu.roll(jnp.where(lane == 127, before, here), 1, 1)
        return ahead - behind

    def coefficients(band):
        rows = pl.ds(pl.multiple_of(8 * band, 8), 8)
        for j in range(6):
            wet = F[WT, j, rows, :]
            mass = F[MA, j, rows, :]
            cover = F[CO, j, rows, :]
            g = wet / (mass + F[DR, j, rows, :] + 1.0 - wet)
            push = g * cover
            F[MA, j, rows, :] = g * mass
            F[WX, j, rows, :] = push * F[WX, j, rows, :]
            F[WY, j, rows, :] = push * F[WY, j, rows, :]
            F[DR, j, rows, :] = 0.25 * g
            F[WT, j, rows, :] = wet * (1.0 / 3.0)

    def stress(band, last=None):
        row = pl.multiple_of(8 * band, 8)
        rows, above, below = pl.ds(row, 8), pl.ds(row - 1, 8), pl.ds(row + 1, 8)
        for j in range(6):
            before, after = (j + 5) % 6, (j + 1) % 6
            ux = right_less_left(F[U, before, rows, :], F[U, j, rows, :], F[U, after, rows, :])
            vx = right_less_left(F[V, before, rows, :], F[V, j, rows, :], F[V, after, rows, :])
            uy = F[U, j, below, :] - F[U, j, above, :]
            vy = F[V, j, below, :] - F[V, j, above, :]
            div, ten, shr = ux + vy, ux - vy, uy + vx
            square = 0.25 * (div * div + 0.25 * (ten * ten + shr * shr)) + 0.0025
            strength = F[ST, j, rows, :]
            half = strength * lax.rsqrt(square)
            eighth = 0.25 * half
            third = F[WT, j, rows, :]
            s1 = third * (F[S1, j, rows, :] + half * div - 2.0 * strength)
            s2 = third * (F[S2, j, rows, :] + eighth * ten)
            s12 = third * (F[S12, j, rows, :] + eighth * shr)
            F[S1, j, rows, :] = s1
            F[S2, j, rows, :] = s2
            F[S12, j, rows, :] = s12
            if last is not None and j < TILES:
                place = (pl.ds(last, 8), pl.ds(j * 128, 128))
                out[(S1, *place)] = s1
                out[(S2, *place)] = s2
                out[(S12, *place)] = s12

    def momentum(band, last=None):
        row = pl.multiple_of(8 * band, 8)
        rows, above, below = pl.ds(row, 8), pl.ds(row - 1, 8), pl.ds(row + 1, 8)
        for j in range(6):
            around = ((j + 5) % 6, j, (j + 1) % 6)
            px = right_less_left(*(F[S1, k, rows, :] + F[S2, k, rows, :] for k in around))
            cx = right_less_left(*(F[S12, k, rows, :] for k in around))
            cy = F[S12, j, below, :] - F[S12, j, above, :]
            my = (F[S1, j, below, :] - F[S2, j, below, :]) - (F[S1, j, above, :] - F[S2, j, above, :])
            a, g = F[MA, j, rows, :], F[DR, j, rows, :]
            u, v = F[U, j, rows, :], F[V, j, rows, :]
            next_u = a * (u + 0.5 * v) + g * (px + 2.0 * cy) + F[WX, j, rows, :]
            next_v = a * (v - 0.5 * u) + g * (2.0 * cx + my) + F[WY, j, rows, :]
            if last is None:
                F[U, j, rows, :] = next_u
                F[V, j, rows, :] = next_v
            elif j < TILES:
                place = (pl.ds(last, 8), pl.ds(j * 128, 128))
                out[(U, *place)] = next_u
                out[(V, *place)] = next_v

    def half_stage(lag, band):
        last = None
        if lag >= 6:
            row = 8 * (band - FIRST - 1)
            last = max(row, 0) if isinstance(band, int) else pl.multiple_of(jnp.maximum(row, 0), 8)
            if isinstance(band, int) and band == LAST:
                last = None
        (momentum if lag % 2 else stress)(band, last)

    def step(t, carry):
        coefficients(t + FIRST)
        for lag in range(8):
            half_stage(lag, t + (FIRST - lag))
        return carry

    weights.wait()
    wait_load(0)
    sums(0, 0)
    enter()
    edge(0).start()
    start_fields()
    start_load(4)
    start_load(5)
    wait_load(1)
    sums(15, 0)
    edge(1).start()
    wait_load(2)
    lax.fori_loop(1, 4, sums, 0)
    for c in range(3):
        border(c).start()
    inner(0).start()
    wait_load(3)
    lax.fori_loop(4, 8, sums, 0)
    border(3).start()
    border(4).start()

    wait_fields()

    def given(block, carry):
        row = pl.multiple_of(block * 16, 16)
        for j in range(TILES):
            F[WT, j, pl.ds(row + TOP_ROW, 16), :] = LAND[pl.ds(row, 16), pl.ds(j * 128, 128)].astype(jnp.float32)
        pack(0, 9, LS, row, 16)
        return carry

    lax.fori_loop(0, 16, given, 0)

    @pl.when(even)
    def _():
        pl.semaphore_wait(near, 2)

    for d in range(2):
        remote(LS.at[d], LR.at[d], edge_send, edge_recv, sides[d]).start()

    def to_rows(k):
        @pl.when(has_up)
        def _():
            lat_message(0, k).start()

        @pl.when(has_down)
        def _():
            lat_message(1, k).start()

    to_rows(0)

    for k in range(2):
        edge(k).wait_recv()
        totals(range(5), 248 * k, 8)
        pack(ST, 3, XS, 248 * k, 8)
        start_columns(248 * k, 8, CHUNKS + k)
    to_rows(1)
    inner(1).start()
    border(5).start()
    wait_load(4)
    wait_load(5)
    lax.fori_loop(8, 15, sums, 0)

    remote(LS, LR, edge_send, edge_recv, sides[0]).wait_recv()

    def take(block, carry):
        unpack(0, 9, LR, pl.multiple_of(block * 16, 16), 16)
        return carry

    lax.fori_loop(0, 16, take, 0)
    for k in range(2):
        wait_columns(248 * k, 8, CHUNKS + k)
        unpack(ST, 3, XR, 248 * k, 8)
    to_rows(2)
    for c in range(3):
        border(2 * c + 6).start()
        border(2 * c + 7).start()
        inner(c + 2).start()
    inner(5).start()

    def columns(c):
        row = pl.multiple_of(8 + c * 16, 8)
        border(c).wait_recv()
        totals(range(2), row, 16)
        pack(ST, 3, XS, row, 16)
        start_columns(row, 16, c)

    for c in range(COLUMNS_AHEAD):
        columns(c)

    everything = (slice(None), slice(None))

    @pl.when(has_down)
    def _():
        lat_copy(0, *everything).wait_recv()
        lat_copy(1, *everything).wait_send()

    @pl.when(has_up)
    def _():
        lat_copy(1, *everything).wait_recv()
        lat_copy(0, *everything).wait_send()

    lax.fori_loop(0, 2, step, 0)

    def columns_here(c):
        row = pl.multiple_of(8 + c * 16, 8)
        wait_columns(row, 16, c)
        unpack(ST, 3, XR, row, 16)

    def chunk(c, carry):
        @pl.when(c + COLUMNS_AHEAD < CHUNKS)
        def _():
            columns(c + COLUMNS_AHEAD)

        columns_here(c)
        inner(c).wait_recv()

        @pl.when(c + BORDERS_AHEAD < CHUNKS)
        def _():
            border(c + BORDERS_AHEAD).start()

        @pl.when(c + INNERS_AHEAD < CHUNKS - 1)
        def _():
            inner(c + INNERS_AHEAD).start()

        @pl.when(c + INNERS_AHEAD == CHUNKS - 1)
        def _():
            last_inner(0).start()
            last_inner(1).start()

        totals(range(2, 5), pl.multiple_of(8 + c * 16, 8), 16)
        lax.fori_loop(2 * c + 2, 2 * c + 4, step, 0)
        return carry

    lax.fori_loop(0, CHUNKS - 1, chunk, 0)
    columns_here(CHUNKS - 1)
    last_inner(0).wait_recv()
    totals(range(2, 5), ROWS - 24, 8)
    lax.fori_loop(30, 31, step, 0)
    last_inner(1).wait_recv()
    totals(range(2, 5), ROWS - 16, 8)
    lax.fori_loop(31, 34, step, 0)
    for t in range(34, 40):
        for lag in range(t - 33, 8):
            half_stage(lag, t + FIRST - lag)

    remote(PT, QT, cat_send, cat_recv.at[0], peer).wait_send()
    remote(XS, XR, lon_send, lon_recv.at[0], sides[0]).wait_send()
    remote(LS, LR, edge_send, edge_recv, sides[0]).wait_send()


def shards(*arrays):
    dma = pltpu.SemaphoreType.DMA
    f32 = jnp.float32
    result = pl.pallas_call(
        kernel,
        out_shape=jax.ShapeDtypeStruct((5, ROWS, COLS), f32),
        in_specs=[pl.BlockSpec(memory_space=pltpu.HBM)] * len(arrays),
        out_specs=pl.BlockSpec(memory_space=pltpu.VMEM),
        scratch_shapes=[
            pltpu.VMEM((12, 6, HEIGHT, 128), f32),
            pltpu.SMEM((NCAT,), f32),
            pltpu.VMEM((2, NCAT, ROWS, COLS), jnp.bfloat16),
            pltpu.VMEM((ROWS, COLS), jnp.int32),
            pltpu.VMEM((ROWS, COLS), jnp.int32),
            pltpu.VMEM((3, TILES, ROWS, 128), f32),
            pltpu.VMEM((3, TILES, ROWS, 128), f32),
            pltpu.VMEM((2, ROWS, 128), f32),
            pltpu.VMEM((2, ROWS, 128), f32),
            pltpu.VMEM((2, ROWS, 128), f32),
            pltpu.VMEM((2, ROWS, 128), f32),
            dma,
            dma((2 * CHUNKS + 3,)),
            dma,
            dma((CHUNKS + 2,)),
            dma,
            dma,
            dma((2,)),
            dma((2,)),
            dma((len(LOADS),)),
            dma((len(TOPS),)),
            dma((3,)),
            pltpu.SemaphoreType.REGULAR,
        ],
        compiler_params=pltpu.CompilerParams(
            collective_id=0, has_side_effects=True, vmem_limit_bytes=44 * 2**20
        ),
        name="ice",
    )(*(pltpu.with_memory_space_constraint(a, pltpu.HBM) for a in arrays))
    return tuple(result[i] for i in range(5))


def solution(mesh):
    block = P("cat", "lat", "lon")
    plane = P("lat", "lon")
    return jax.shard_map(
        shards,
        mesh=mesh,
        in_specs=(block, block, P("cat"), *[plane] * 10),
        out_specs=(plane,) * 5,
        check_vma=False,
    )
```

```python
import jax
import jax.numpy as jnp
from jax import lax
from jax.experimental import pallas as pl
from jax.experimental.pallas import tpu as pltpu
from jax.sharding import PartitionSpec as P

U, V, S1, S2, S12, WX, WY, DR, WT, ST, MA, CO = range(12)
NCAT = 20
ROWS = 256
COLS = 640
TILES = 5
CHUNKS = 15
COLUMNS_AHEAD = 6
BORDERS_AHEAD = 12
INNERS_AHEAD = 6
ORDER = (0, 4, 1, 2, 3)
TOP_ROW = 72
HEIGHT = 344
FIRST, LAST = 8, 41
LOADS = ((0, 16), (240, 16), (16, 48), (64, 64), (128, 64), (192, 48))
TOPS = ((0, 16), (240, 16), (16, 224))
MESH = pl.DeviceIdType.MESH


def kernel(th, ar, weight, top, land, u0, v0, d0, t0, h0, wx0, wy0, dr0, out,
           F, W, TA, TOP, LAND, PT, QT, LS, LR, XS, XR,
           cat_send, cat_recv, lon_send, lon_recv, edge_send, edge_recv, lat_send, lat_recv,
           load_sem, top_sem, field_sem, near):
    cat, lat, lon = lax.axis_index("cat"), lax.axis_index("lat"), lax.axis_index("lon")
    peer = (1 - cat, lat, lon)
    sides = ((cat, lat, lax.rem(lon + 15, 16)), (cat, lat, lax.rem(lon + 1, 16)))
    up = (cat, lax.rem(lat + 3, 4), lon)
    down = (cat, lax.rem(lat + 1, 4), lon)
    cross_up = (1 - cat, lax.rem(lat + 3, 4), lon)
    cross_down = (1 - cat, lax.rem(lat + 1, 4), lon)
    has_up, has_down = lat > 0, lat < 3

    even = lax.rem(lon, 2) == 0

    def load_rows(i):
        return pl.ds(*LOADS[i])

    def start_load(i):
        rows = load_rows(i)
        if i < len(TOPS):
            some = pl.ds(*TOPS[i])
            pltpu.make_async_copy(top.at[some, :], TOP.at[some, :], top_sem.at[i]).start()
        for k, ref in enumerate((th, ar)):
            pltpu.make_async_copy(ref.at[:, rows, :], TA.at[k, :, rows, :], load_sem.at[i]).start()

    def wait_load(i):
        if i < len(TOPS):
            some = TOP.at[pl.ds(*TOPS[i]), :]
            pltpu.make_async_copy(some, some, top_sem.at[i]).wait()
        both = TA.at[:, :, load_rows(i), :]
        pltpu.make_async_copy(both, both, load_sem.at[i]).wait()

    lands = pltpu.make_async_copy(land, LAND, field_sem.at[1])
    weights = pltpu.make_async_copy(weight, W, field_sem.at[2])

    def start_fields():
        for f, ref in enumerate((u0, v0, d0, t0, h0, wx0, wy0, dr0)):
            for j in range(TILES):
                pltpu.make_async_copy(
                    ref.at[:, pl.ds(j * 128, 128)], F.at[f, j, pl.ds(TOP_ROW, ROWS), :], field_sem.at[0]
                ).start()
        lands.start()

    def wait_fields():
        given = F.at[pl.ds(0, 8), pl.ds(0, TILES), pl.ds(TOP_ROW, ROWS), :]
        pltpu.make_async_copy(given, given, field_sem.at[0]).wait()
        lands.wait()

    start_load(0)
    weights.start()
    start_load(1)
    barrier = pltpu.get_barrier_semaphore()
    for device in (peer, up, down, cross_up, cross_down):
        pl.semaphore_signal(barrier, inc=1, device_id=device, device_id_type=MESH)

    @pl.when(even)
    def _():
        for device in sides:
            pl.semaphore_signal(barrier, inc=1, device_id=device, device_id_type=MESH)

    def enter():
        @pl.when(even)
        def _():
            pl.semaphore_wait(barrier, 5)

        @pl.when(jnp.logical_not(even))
        def _():
            pl.semaphore_wait(barrier, 7)
            for device in sides:
                pl.semaphore_signal(near, inc=1, device_id=device, device_id_type=MESH)

    start_load(2)
    start_load(3)

    @pl.when(lat == 0)
    def _():
        F[:, :, pl.ds(8 * FIRST, 8), :] = jnp.zeros((12, 6, 8, 128), jnp.float32)

    @pl.when(lat == 3)
    def _():
        F[:, :, pl.ds(8 * LAST, 8), :] = jnp.zeros((12, 6, 8, 128), jnp.float32)

    lane = lax.broadcasted_iota(jnp.int32, (8, 128), 1)
    lane16 = lax.broadcasted_iota(jnp.int32, (16, 128), 1)
    base = cat * NCAT

    def sums(block, carry):
        rows = pl.ds(pl.multiple_of(block * 16, 16), 16)
        for place, j in enumerate(ORDER):
            cols = pl.ds(j * 128, 128)
            limit = TOP[rows, cols] - base
            strength = jnp.zeros((16, 128), jnp.float32)
            mass = jnp.zeros((16, 128), jnp.float32)
            cover = jnp.zeros((16, 128), jnp.float32)
            for n in range(NCAT):
                h = TA[0, n, rows, cols].astype(jnp.float32)
                c = TA[1, n, rows, cols].astype(jnp.float32)
                c = jnp.where(limit > n, c, 0.0)
                m = c * h
                cover = cover + c
                mass = mass + m
                strength = strength + (W[n] * h) * m
            PT[0, place, rows, :] = strength
            PT[1, place, rows, :] = mass
            PT[2, place, rows, :] = cover
        return carry

    def remote(src, dst, send, recv, device):
        return pltpu.make_async_remote_copy(
            src_ref=src, dst_ref=dst, send_sem=send, recv_sem=recv, device_id=device, device_id_type=MESH
        )

    def cat_message(tiles, rows, k):
        where = (slice(None), tiles, rows, slice(None))
        return remote(PT.at[where], QT.at[where], cat_send, cat_recv.at[k], peer)

    def border(c):
        return cat_message(pl.ds(0, 2), pl.ds(pl.multiple_of(8 + c * 16, 8), 16), c)

    def inner(c):
        return cat_message(pl.ds(2, 3), pl.ds(pl.multiple_of(8 + c * 16, 8), 16), CHUNKS + c)

    def last_inner(k):
        return cat_message(pl.ds(2, 3), pl.ds(ROWS - 24 + 8 * k, 8), 2 * CHUNKS - 1 + k)

    def edge(k):
        return cat_message(pl.ds(0, 5), pl.ds(248 * k, 8), 2 * CHUNKS + 1 + k)

    def start_columns(start, size, k):
        rows = pl.ds(start, size)
        for d in range(2):
            remote(XS.at[d, rows, :], XR.at[d, rows, :], lon_send, lon_recv.at[k], sides[d]).start()

    def wait_columns(start, size, k):
        rows = pl.ds(start, size)
        remote(XS.at[:, rows, :], XR.at[:, rows, :], lon_send, lon_recv.at[k], sides[0]).wait_recv()

    def lat_copy(d, fields, tiles, over=False):
        here, there, device = ((FIRST + 1, LAST, (up, cross_up)[over]), (LAST - 1, FIRST, (down, cross_down)[over]))[d]
        return remote(
            F.at[fields, tiles, pl.ds(8 * here, 8), :], F.at[fields, tiles, pl.ds(8 * there, 8), :],
            lat_send.at[d], lat_recv.at[d], device,
        )

    def to_rows(k):
        fields = (pl.ds(0, 9), pl.ds(9, 3), pl.ds(0, 12))[k]
        corner = pl.ds(TILES, 1)
        for d in range(2):
            crosses = lat == (2, 1)[d]

            @pl.when((has_up, has_down)[d] & jnp.logical_not(crosses))
            def _():
                lat_copy(d, fields, corner if k == 2 else pl.ds(0, TILES)).start()

            if k < 2:
                @pl.when(crosses & (cat == 0))
                def _():
                    for over in range(2):
                        lat_copy(d, fields, pl.ds(0, 3), over).start()

            @pl.when(crosses & (cat == 1))
            def _():
                for over in range(2):
                    lat_copy(d, fields, corner if k == 2 else pl.ds(3, 2), over).start()

    def pack(first, count, send, row, size):
        iota = lane if size == 8 else lane16
        rows = pl.ds(row, size)
        from_rows = pl.ds(row + TOP_ROW, size)
        left = jnp.zeros((size, 128), jnp.float32)
        right = jnp.zeros((size, 128), jnp.float32)
        for i in range(count):
            mine = (iota >= 8 * i) & (iota < 8 * i + 8)
            a = F[first + i, 0, from_rows, :]
            b = F[first + i, 4, from_rows, :]
            left = jnp.where(mine, pltpu.roll(a, 8 * i, 1) if i else a, left)
            right = jnp.where(mine, pltpu.roll(b, 8 * i + 8, 1), right)
        send[0, rows, :] = left
        send[1, rows, :] = right

    def unpack(first, count, recv, row, size):
        iota = lane if size == 8 else lane16
        rows = pl.ds(row, size)
        a = recv[0, rows, :]
        b = recv[1, rows, :]
        for i in range(count):
            ahead = pltpu.roll(a, 128 - 8 * i, 1) if i else a
            behind = pltpu.roll(b, 120 - 8 * i, 1)
            F[first + i, 5, pl.ds(row + TOP_ROW, size), :] = jnp.where(
                iota < 8, ahead, jnp.where(iota >= 120, behind, 0.0)
            )

    def totals(places, row, size):
        for place in places:
            for f in range(3):
                F[ST + f, ORDER[place], pl.ds(row + TOP_ROW, size), :] = (
                    PT[f, place, pl.ds(row, size), :] + QT[f, place, pl.ds(row, size), :]
                )

    def right_less_left(before, here, after):
        ahead = pltpu.roll(jnp.where(lane == 0, after, here), 127, 1)
        behind = pltpu.roll(jnp.where(lane == 127, before, here), 1, 1)
        return ahead - behind

    def coefficients(band):
        rows = pl.ds(pl.multiple_of(8 * band, 8), 8)
        for j in range(6):
            wet = F[WT, j, rows, :]
            mass = F[MA, j, rows, :]
            cover = F[CO, j, rows, :]
            g = wet / (mass + F[DR, j, rows, :] + 1.0 - wet)
            push = g * cover
            F[MA, j, rows, :] = g * mass
            F[WX, j, rows, :] = push * F[WX, j, rows, :]
            F[WY, j, rows, :] = push * F[WY, j, rows, :]
            F[DR, j, rows, :] = 0.25 * g
            F[WT, j, rows, :] = wet * (1.0 / 3.0)
            F[ST, j, rows, :] = (wet * (2.0 / 3.0)) * F[ST, j, rows, :]

    def stress(band, last=None):
        row = pl.multiple_of(8 * band, 8)
        rows, above, below = pl.ds(row, 8), pl.ds(row - 1, 8), pl.ds(row + 1, 8)
        for j in range(6):
            before, after = (j + 5) % 6, (j + 1) % 6
            ux = right_less_left(F[U, before, rows, :], F[U, j, rows, :], F[U, after, rows, :])
            vx = right_less_left(F[V, before, rows, :], F[V, j, rows, :], F[V, after, rows, :])
            uy = F[U, j, below, :] - F[U, j, above, :]
            vy = F[V, j, below, :] - F[V, j, above, :]
            div, ten, shr = ux + vy, ux - vy, uy + vx
            square = div * div + 0.25 * (ten * ten + shr * shr) + 0.01
            strength = F[ST, j, rows, :]
            half = strength * lax.rsqrt(square)
            eighth = 0.25 * half
            third = F[WT, j, rows, :]
            s1 = third * F[S1, j, rows, :] + (half * div - strength)
            s2 = third * F[S2, j, rows, :] + eighth * ten
            s12 = third * F[S12, j, rows, :] + eighth * shr
            F[S1, j, rows, :] = s1
            F[S2, j, rows, :] = s2
            F[S12, j, rows, :] = s12
            if last is not None and j < TILES:
                place = (pl.ds(last, 8), pl.ds(j * 128, 128))
                out[(S1, *place)] = s1
                out[(S2, *place)] = s2
                out[(S12, *place)] = s12

    def momentum(band, last=None):
        row = pl.multiple_of(8 * band, 8)
        rows, above, below = pl.ds(row, 8), pl.ds(row - 1, 8), pl.ds(row + 1, 8)
        for j in range(6):
            around = ((j + 5) % 6, j, (j + 1) % 6)
            px = right_less_left(*(F[S1, k, rows, :] + F[S2, k, rows, :] for k in around))
            cx = right_less_left(*(F[S12, k, rows, :] for k in around))
            cy = F[S12, j, below, :] - F[S12, j, above, :]
            my = (F[S1, j, below, :] - F[S2, j, below, :]) - (F[S1, j, above, :] - F[S2, j, above, :])
            a, g = F[MA, j, rows, :], F[DR, j, rows, :]
            u, v = F[U, j, rows, :], F[V, j, rows, :]
            next_u = a * (u + 0.5 * v) + g * (px + 2.0 * cy) + F[WX, j, rows, :]
            next_v = a * (v - 0.5 * u) + g * (2.0 * cx + my) + F[WY, j, rows, :]
            if last is None:
                F[U, j, rows, :] = next_u
                F[V, j, rows, :] = next_v
            elif j < TILES:
                place = (pl.ds(last, 8), pl.ds(j * 128, 128))
                out[(U, *place)] = next_u
                out[(V, *place)] = next_v

    def half_stage(lag, band):
        last = None
        if lag >= 6:
            row = 8 * (band - FIRST - 1)
            last = max(row, 0) if isinstance(band, int) else pl.multiple_of(jnp.maximum(row, 0), 8)
            if isinstance(band, int) and band == LAST:
                last = None
        (momentum if lag % 2 else stress)(band, last)

    def step(t, carry):
        coefficients(t + FIRST)
        for lag in range(8):
            half_stage(lag, t + (FIRST - lag))
        return carry

    weights.wait()
    wait_load(0)
    sums(0, 0)
    enter()
    edge(0).start()
    start_fields()
    start_load(4)
    start_load(5)
    wait_load(1)
    sums(15, 0)
    edge(1).start()
    wait_load(2)
    lax.fori_loop(1, 4, sums, 0)
    for c in range(3):
        border(c).start()
    inner(0).start()
    wait_load(3)
    lax.fori_loop(4, 8, sums, 0)
    border(3).start()
    border(4).start()

    wait_fields()

    def given(block, carry):
        row = pl.multiple_of(block * 16, 16)
        for j in range(TILES):
            F[WT, j, pl.ds(row + TOP_ROW, 16), :] = LAND[pl.ds(row, 16), pl.ds(j * 128, 128)].astype(jnp.float32)
        pack(0, 9, LS, row, 16)
        return carry

    lax.fori_loop(0, 16, given, 0)

    @pl.when(even)
    def _():
        pl.semaphore_wait(near, 2)

    for d in range(2):
        remote(LS.at[d], LR.at[d], edge_send, edge_recv, sides[d]).start()

    to_rows(0)

    for k in range(2):
        edge(k).wait_recv()
        totals(range(5), 248 * k, 8)
        pack(ST, 3, XS, 248 * k, 8)
        start_columns(248 * k, 8, CHUNKS + k)
    to_rows(1)
    inner(1).start()
    border(5).start()
    wait_load(4)
    wait_load(5)
    lax.fori_loop(8, 15, sums, 0)

    border(6).start()
    border(7).start()
    inner(2).start()
    remote(LS, LR, edge_send, edge_recv, sides[0]).wait_recv()

    def take(block, carry):
        unpack(0, 9, LR, pl.multiple_of(block * 16, 16), 16)
        return carry

    lax.fori_loop(0, 16, take, 0)
    for k in range(2):
        wait_columns(248 * k, 8, CHUNKS + k)
        unpack(ST, 3, XR, 248 * k, 8)
    to_rows(2)
    for c in range(2):
        border(2 * c + 8).start()
        border(2 * c + 9).start()
        inner(c + 3).start()
    inner(5).start()

    def columns(c):
        row = pl.multiple_of(8 + c * 16, 8)
        border(c).wait_recv()
        totals(range(2), row, 16)
        pack(ST, 3, XS, row, 16)
        start_columns(row, 16, c)

    for c in range(COLUMNS_AHEAD):
        columns(c)

    everything = (slice(None), slice(None))

    @pl.when(has_down)
    def _():
        lat_copy(0, *everything).wait_recv()
        lat_copy(1, *everything).wait_send()

    @pl.when(has_up)
    def _():
        lat_copy(1, *everything).wait_recv()
        lat_copy(0, *everything).wait_send()

    lax.fori_loop(0, 2, step, 0)

    def columns_here(c):
        row = pl.multiple_of(8 + c * 16, 8)
        wait_columns(row, 16, c)
        unpack(ST, 3, XR, row, 16)

    def chunk(c, carry):
        @pl.when(c + COLUMNS_AHEAD < CHUNKS)
        def _():
            columns(c + COLUMNS_AHEAD)

        columns_here(c)
        inner(c).wait_recv()

        @pl.when(c + BORDERS_AHEAD < CHUNKS)
        def _():
            border(c + BORDERS_AHEAD).start()

        @pl.when(c + INNERS_AHEAD < CHUNKS - 1)
        def _():
            inner(c + INNERS_AHEAD).start()

        @pl.when(c + INNERS_AHEAD == CHUNKS - 1)
        def _():
            last_inner(0).start()
            last_inner(1).start()

        totals(range(2, 5), pl.multiple_of(8 + c * 16, 8), 16)
        lax.fori_loop(2 * c + 2, 2 * c + 4, step, 0)
        return carry

    lax.fori_loop(0, CHUNKS - 1, chunk, 0)
    columns_here(CHUNKS - 1)
    last_inner(0).wait_recv()
    totals(range(2, 5), ROWS - 24, 8)
    lax.fori_loop(30, 31, step, 0)
    last_inner(1).wait_recv()
    totals(range(2, 5), ROWS - 16, 8)
    lax.fori_loop(31, 34, step, 0)
    for t in range(34, 40):
        for lag in range(t - 33, 8):
            half_stage(lag, t + FIRST - lag)

    remote(PT, QT, cat_send, cat_recv.at[0], peer).wait_send()
    remote(XS, XR, lon_send, lon_recv.at[0], sides[0]).wait_send()
    remote(LS, LR, edge_send, edge_recv, sides[0]).wait_send()


def shards(*arrays):
    dma = pltpu.SemaphoreType.DMA
    f32 = jnp.float32
    result = pl.pallas_call(
        kernel,
        out_shape=jax.ShapeDtypeStruct((5, ROWS, COLS), f32),
        in_specs=[pl.BlockSpec(memory_space=pltpu.HBM)] * len(arrays),
        out_specs=pl.BlockSpec(memory_space=pltpu.VMEM),
        scratch_shapes=[
            pltpu.VMEM((12, 6, HEIGHT, 128), f32),
            pltpu.SMEM((NCAT,), f32),
            pltpu.VMEM((2, NCAT, ROWS, COLS), jnp.bfloat16),
            pltpu.VMEM((ROWS, COLS), jnp.int32),
            pltpu.VMEM((ROWS, COLS), jnp.int32),
            pltpu.VMEM((3, TILES, ROWS, 128), f32),
            pltpu.VMEM((3, TILES, ROWS, 128), f32),
            pltpu.VMEM((2, ROWS, 128), f32),
            pltpu.VMEM((2, ROWS, 128), f32),
            pltpu.VMEM((2, ROWS, 128), f32),
            pltpu.VMEM((2, ROWS, 128), f32),
            dma,
            dma((2 * CHUNKS + 3,)),
            dma,
            dma((CHUNKS + 2,)),
            dma,
            dma,
            dma((2,)),
            dma((2,)),
            dma((len(LOADS),)),
            dma((len(TOPS),)),
            dma((3,)),
            pltpu.SemaphoreType.REGULAR,
        ],
        compiler_params=pltpu.CompilerParams(
            collective_id=0, has_side_effects=True, vmem_limit_bytes=44 * 2**20
        ),
        name="ice",
    )(*(pltpu.with_memory_space_constraint(a, pltpu.HBM) for a in arrays))
    return tuple(result[i] for i in range(5))


def solution(mesh):
    block = P("cat", "lat", "lon")
    plane = P("lat", "lon")
    return jax.shard_map(
        shards,
        mesh=mesh,
        in_specs=(block, block, P("cat"), *[plane] * 10),
        out_specs=(plane,) * 5,
        check_vma=False,
    )
```

```python
import jax
import jax.numpy as jnp
from jax import lax
from jax.experimental import pallas as pl
from jax.experimental.pallas import tpu as pltpu
from jax.sharding import PartitionSpec as P

U, V, S1, S2, S12, WX, WY, DR, WT, ST, MA, CO = range(12)
NCAT = 20
ROWS = 256
COLS = 640
TILES = 5
CHUNKS = 15
COLUMNS_AHEAD = 6
BORDERS_AHEAD = 12
INNERS_AHEAD = 6
ORDER = (0, 4, 1, 2, 3)
TOP_ROW = 72
HEIGHT = 344
FIRST, LAST = 8, 41
LOADS = ((0, 16), (240, 16), (16, 48), (64, 64), (128, 64), (192, 48))
TOPS = ((0, 16), (240, 16), (16, 224))
MESH = pl.DeviceIdType.MESH


def kernel(th, ar, weight, top, land, u0, v0, d0, t0, h0, wx0, wy0, dr0, out,
           F, W, TA, TOP, LAND, PT, QT, LS, LR, XS, XR, HS, HR,
           cat_send, cat_recv, lon_send, lon_recv, edge_send, edge_recv, lat_send, lat_recv, halo_send, halo_recv,
           load_sem, top_sem, field_sem, near):
    cat, lat, lon = lax.axis_index("cat"), lax.axis_index("lat"), lax.axis_index("lon")
    peer = (1 - cat, lat, lon)
    sides = ((cat, lat, lax.rem(lon + 15, 16)), (cat, lat, lax.rem(lon + 1, 16)))
    up = (cat, lax.rem(lat + 3, 4), lon)
    down = (cat, lax.rem(lat + 1, 4), lon)
    cross_up = (1 - cat, lax.rem(lat + 3, 4), lon)
    cross_down = (1 - cat, lax.rem(lat + 1, 4), lon)
    has_up, has_down = lat > 0, lat < 3

    even = lax.rem(lon, 2) == 0

    def load_rows(i):
        return pl.ds(*LOADS[i])

    def start_load(i):
        rows = load_rows(i)
        if i < len(TOPS):
            some = pl.ds(*TOPS[i])
            pltpu.make_async_copy(top.at[some, :], TOP.at[some, :], top_sem.at[i]).start()
        for k, ref in enumerate((th, ar)):
            pltpu.make_async_copy(ref.at[:, rows, :], TA.at[k, :, rows, :], load_sem.at[i]).start()

    def wait_load(i):
        if i < len(TOPS):
            some = TOP.at[pl.ds(*TOPS[i]), :]
            pltpu.make_async_copy(some, some, top_sem.at[i]).wait()
        both = TA.at[:, :, load_rows(i), :]
        pltpu.make_async_copy(both, both, load_sem.at[i]).wait()

    lands = pltpu.make_async_copy(land, LAND, field_sem.at[1])
    weights = pltpu.make_async_copy(weight, W, field_sem.at[2])

    def start_fields():
        for f, ref in enumerate((u0, v0, d0, t0, h0, wx0, wy0, dr0)):
            for j in range(TILES):
                pltpu.make_async_copy(
                    ref.at[:, pl.ds(j * 128, 128)], F.at[f, j, pl.ds(TOP_ROW, ROWS), :], field_sem.at[0]
                ).start()
        lands.start()

    def wait_fields():
        given = F.at[pl.ds(0, 8), pl.ds(0, TILES), pl.ds(TOP_ROW, ROWS), :]
        pltpu.make_async_copy(given, given, field_sem.at[0]).wait()
        lands.wait()

    start_load(0)
    weights.start()
    start_load(1)
    barrier = pltpu.get_barrier_semaphore()
    for device in (peer, up, down, cross_up, cross_down):
        pl.semaphore_signal(barrier, inc=1, device_id=device, device_id_type=MESH)

    @pl.when(even)
    def _():
        for device in sides:
            pl.semaphore_signal(barrier, inc=1, device_id=device, device_id_type=MESH)

    def enter():
        @pl.when(even)
        def _():
            pl.semaphore_wait(barrier, 5)

        @pl.when(jnp.logical_not(even))
        def _():
            pl.semaphore_wait(barrier, 7)
            for device in sides:
                pl.semaphore_signal(near, inc=1, device_id=device, device_id_type=MESH)

    start_load(2)
    start_load(3)

    @pl.when(lat == 0)
    def _():
        F[:, :, pl.ds(8 * FIRST, 8), :] = jnp.zeros((12, 6, 8, 128), jnp.float32)

    @pl.when(lat == 3)
    def _():
        F[:, :, pl.ds(8 * LAST, 8), :] = jnp.zeros((12, 6, 8, 128), jnp.float32)

    lane = lax.broadcasted_iota(jnp.int32, (8, 128), 1)
    lane16 = lax.broadcasted_iota(jnp.int32, (16, 128), 1)
    base = cat * NCAT

    def sums(block, carry):
        rows = pl.ds(pl.multiple_of(block * 16, 16), 16)
        for place, j in enumerate(ORDER):
            cols = pl.ds(j * 128, 128)
            limit = TOP[rows, cols] - base
            strength = jnp.zeros((16, 128), jnp.float32)
            mass = jnp.zeros((16, 128), jnp.float32)
            cover = jnp.zeros((16, 128), jnp.float32)
            for n in range(NCAT):
                h = TA[0, n, rows, cols].astype(jnp.float32)
                c = TA[1, n, rows, cols].astype(jnp.float32)
                c = jnp.where(limit > n, c, 0.0)
                m = c * h
                cover = cover + c
                mass = mass + m
                strength = strength + (W[n] * h) * m
            PT[0, place, rows, :] = strength
            PT[1, place, rows, :] = mass
            PT[2, place, rows, :] = cover
        return carry

    def remote(src, dst, send, recv, device):
        return pltpu.make_async_remote_copy(
            src_ref=src, dst_ref=dst, send_sem=send, recv_sem=recv, device_id=device, device_id_type=MESH
        )

    def cat_message(tiles, rows, k):
        where = (slice(None), tiles, rows, slice(None))
        return remote(PT.at[where], QT.at[where], cat_send, cat_recv.at[k], peer)

    def border(c):
        return cat_message(pl.ds(0, 2), pl.ds(pl.multiple_of(8 + c * 16, 8), 16), c)

    def inner(c):
        return cat_message(pl.ds(2, 3), pl.ds(pl.multiple_of(8 + c * 16, 8), 16), CHUNKS + c)

    def last_inner(k):
        return cat_message(pl.ds(2, 3), pl.ds(ROWS - 24 + 8 * k, 8), 2 * CHUNKS - 1 + k)

    def edge(k):
        return cat_message(pl.ds(0, 5), pl.ds(248 * k, 8), 2 * CHUNKS + 1 + k)

    def start_columns(start, size, k):
        rows = pl.ds(start, size)
        for d in range(2):
            remote(XS.at[d, rows, :], XR.at[d, rows, :], lon_send, lon_recv.at[k], sides[d]).start()

    def wait_columns(start, size, k):
        rows = pl.ds(start, size)
        remote(XS.at[:, rows, :], XR.at[:, rows, :], lon_send, lon_recv.at[k], sides[0]).wait_recv()

    def lat_copy(d, fields, tiles, over=False):
        here, there, device = ((FIRST + 1, LAST, (up, cross_up)[over]), (LAST - 1, FIRST, (down, cross_down)[over]))[d]
        return remote(
            F.at[fields, tiles, pl.ds(8 * here, 8), :], F.at[fields, tiles, pl.ds(8 * there, 8), :],
            lat_send.at[d], lat_recv.at[d], device,
        )

    def to_rows(k):
        fields = (pl.ds(0, 9), pl.ds(9, 3))[k]
        halves = (
            (((pl.ds(0, 9), pl.ds(0, 2)), (pl.ds(0, 6), pl.ds(2, 1))), ((pl.ds(0, 9), pl.ds(3, 2)), (pl.ds(6, 3), pl.ds(2, 1)))),
            (((pl.ds(9, 3), pl.ds(0, 2)),), ((pl.ds(9, 3), pl.ds(2, 3)),)),
        )[k]
        for d in range(2):
            crosses = lat == (2, 1)[d]

            @pl.when((has_up, has_down)[d] & jnp.logical_not(crosses))
            def _():
                lat_copy(d, fields, pl.ds(0, TILES)).start()

            for holder in range(2):
                @pl.when(crosses & (cat == holder))
                def _():
                    for some, tiles in halves[holder]:
                        for over in range(2):
                            lat_copy(d, some, tiles, over).start()

    def pack(first, count, send, row, size, place=None):
        iota = lane if size == 8 else lane16
        rows = pl.ds(row if place is None else place, size)
        from_rows = pl.ds(row + TOP_ROW, size)
        left = jnp.zeros((size, 128), jnp.float32)
        right = jnp.zeros((size, 128), jnp.float32)
        for i in range(count):
            mine = (iota >= 8 * i) & (iota < 8 * i + 8)
            a = F[first + i, 0, from_rows, :]
            b = F[first + i, 4, from_rows, :]
            left = jnp.where(mine, pltpu.roll(a, 8 * i, 1) if i else a, left)
            right = jnp.where(mine, pltpu.roll(b, 8 * i + 8, 1), right)
        send[0, rows, :] = left
        send[1, rows, :] = right

    def unpack(first, count, recv, row, size, place=None):
        iota = lane if size == 8 else lane16
        rows = pl.ds(row if place is None else place, size)
        a = recv[0, rows, :]
        b = recv[1, rows, :]
        for i in range(count):
            ahead = pltpu.roll(a, 128 - 8 * i, 1) if i else a
            behind = pltpu.roll(b, 120 - 8 * i, 1)
            F[first + i, 5, pl.ds(row + TOP_ROW, size), :] = jnp.where(
                iota < 8, ahead, jnp.where(iota >= 120, behind, 0.0)
            )

    def totals(places, row, size):
        for place in places:
            for f in range(3):
                F[ST + f, ORDER[place], pl.ds(row + TOP_ROW, size), :] = (
                    PT[f, place, pl.ds(row, size), :] + QT[f, place, pl.ds(row, size), :]
                )

    def right_less_left(before, here, after):
        ahead = pltpu.roll(jnp.where(lane == 0, after, here), 127, 1)
        behind = pltpu.roll(jnp.where(lane == 127, before, here), 1, 1)
        return ahead - behind

    def coefficients(band):
        rows = pl.ds(pl.multiple_of(8 * band, 8), 8)
        for j in range(6):
            wet = F[WT, j, rows, :]
            mass = F[MA, j, rows, :]
            cover = F[CO, j, rows, :]
            g = wet / (mass + F[DR, j, rows, :] + 1.0 - wet)
            push = g * cover
            F[MA, j, rows, :] = g * mass
            F[WX, j, rows, :] = push * F[WX, j, rows, :]
            F[WY, j, rows, :] = push * F[WY, j, rows, :]
            F[DR, j, rows, :] = 0.25 * g
            F[WT, j, rows, :] = wet * (1.0 / 3.0)
            F[ST, j, rows, :] = (wet * (2.0 / 3.0)) * F[ST, j, rows, :]

    def stress(band, last=None):
        row = pl.multiple_of(8 * band, 8)
        rows, above, below = pl.ds(row, 8), pl.ds(row - 1, 8), pl.ds(row + 1, 8)
        for j in range(6):
            before, after = (j + 5) % 6, (j + 1) % 6
            ux = right_less_left(F[U, before, rows, :], F[U, j, rows, :], F[U, after, rows, :])
            vx = right_less_left(F[V, before, rows, :], F[V, j, rows, :], F[V, after, rows, :])
            uy = F[U, j, below, :] - F[U, j, above, :]
            vy = F[V, j, below, :] - F[V, j, above, :]
            div, ten, shr = ux + vy, ux - vy, uy + vx
            square = div * div + 0.25 * (ten * ten + shr * shr) + 0.01
            strength = F[ST, j, rows, :]
            half = strength * lax.rsqrt(square)
            eighth = 0.25 * half
            third = F[WT, j, rows, :]
            s1 = third * F[S1, j, rows, :] + (half * div - strength)
            s2 = third * F[S2, j, rows, :] + eighth * ten
            s12 = third * F[S12, j, rows, :] + eighth * shr
            F[S1, j, rows, :] = s1
            F[S2, j, rows, :] = s2
            F[S12, j, rows, :] = s12
            if last is not None and j < TILES:
                place = (pl.ds(last, 8), pl.ds(j * 128, 128))
                out[(S1, *place)] = s1
                out[(S2, *place)] = s2
                out[(S12, *place)] = s12

    def momentum(band, last=None):
        row = pl.multiple_of(8 * band, 8)
        rows, above, below = pl.ds(row, 8), pl.ds(row - 1, 8), pl.ds(row + 1, 8)
        for j in range(6):
            around = ((j + 5) % 6, j, (j + 1) % 6)
            px = right_less_left(*(F[S1, k, rows, :] + F[S2, k, rows, :] for k in around))
            cx = right_less_left(*(F[S12, k, rows, :] for k in around))
            cy = F[S12, j, below, :] - F[S12, j, above, :]
            my = (F[S1, j, below, :] - F[S2, j, below, :]) - (F[S1, j, above, :] - F[S2, j, above, :])
            a, g = F[MA, j, rows, :], F[DR, j, rows, :]
            u, v = F[U, j, rows, :], F[V, j, rows, :]
            next_u = a * (u + 0.5 * v) + g * (px + 2.0 * cy) + F[WX, j, rows, :]
            next_v = a * (v - 0.5 * u) + g * (2.0 * cx + my) + F[WY, j, rows, :]
            if last is None:
                F[U, j, rows, :] = next_u
                F[V, j, rows, :] = next_v
            elif j < TILES:
                place = (pl.ds(last, 8), pl.ds(j * 128, 128))
                out[(U, *place)] = next_u
                out[(V, *place)] = next_v

    def half_stage(lag, band):
        last = None
        if lag >= 6:
            row = 8 * (band - FIRST - 1)
            last = max(row, 0) if isinstance(band, int) else pl.multiple_of(jnp.maximum(row, 0), 8)
            if isinstance(band, int) and band == LAST:
                last = None
        (momentum if lag % 2 else stress)(band, last)

    def step(t, carry):
        coefficients(t + FIRST)
        for lag in range(8):
            half_stage(lag, t + (FIRST - lag))
        return carry

    weights.wait()
    wait_load(0)
    sums(0, 0)
    enter()
    edge(0).start()
    start_fields()
    start_load(4)
    start_load(5)
    wait_load(1)
    sums(15, 0)
    edge(1).start()
    wait_load(2)
    lax.fori_loop(1, 4, sums, 0)
    for c in range(3):
        border(c).start()
    inner(0).start()
    wait_load(3)
    lax.fori_loop(4, 8, sums, 0)
    border(3).start()
    border(4).start()

    wait_fields()

    def given(block, carry):
        row = pl.multiple_of(block * 16, 16)
        for j in range(TILES):
            F[WT, j, pl.ds(row + TOP_ROW, 16), :] = LAND[pl.ds(row, 16), pl.ds(j * 128, 128)].astype(jnp.float32)
        pack(0, 9, LS, row, 16)
        return carry

    lax.fori_loop(0, 16, given, 0)

    @pl.when(even)
    def _():
        pl.semaphore_wait(near, 2)

    for d in range(2):
        remote(LS.at[d], LR.at[d], edge_send, edge_recv, sides[d]).start()

    to_rows(0)

    for k in range(2):
        edge(k).wait_recv()
        totals(range(5), 248 * k, 8)
        pack(ST, 3, XS, 248 * k, 8)
        start_columns(248 * k, 8, CHUNKS + k)
    to_rows(1)
    inner(1).start()
    border(5).start()
    wait_load(4)
    wait_load(5)
    lax.fori_loop(8, 15, sums, 0)

    for c in range(3):
        border(2 * c + 6).start()
        border(2 * c + 7).start()
        inner(c + 2).start()
    inner(5).start()
    remote(LS, LR, edge_send, edge_recv, sides[0]).wait_recv()

    def take(block, carry):
        unpack(0, 9, LR, pl.multiple_of(block * 16, 16), 16)
        return carry

    lax.fori_loop(0, 16, take, 0)
    for k in range(2):
        wait_columns(248 * k, 8, CHUNKS + k)
        unpack(ST, 3, XR, 248 * k, 8)

    def columns(c):
        row = pl.multiple_of(8 + c * 16, 8)
        border(c).wait_recv()
        totals(range(2), row, 16)
        pack(ST, 3, XS, row, 16)
        start_columns(row, 16, c)

    for c in range(3):
        columns(c)
    halo = (slice(None), pl.ds(0, TILES))

    @pl.when(has_down)
    def _():
        lat_copy(0, *halo).wait_recv()
        lat_copy(1, *halo).wait_send()

    @pl.when(has_up)
    def _():
        lat_copy(1, *halo).wait_recv()
        lat_copy(0, *halo).wait_send()

    for k in range(2):
        pack(0, 12, HS, (-8, ROWS)[k], 8, 8 * k)
    for d in range(2):
        remote(HS.at[d], HR.at[d], halo_send, halo_recv, sides[d]).start()
    for c in range(3, COLUMNS_AHEAD):
        columns(c)
    remote(HS, HR, halo_send, halo_recv, sides[0]).wait_recv()
    for k in range(2):
        unpack(0, 12, HR, (-8, ROWS)[k], 8, 8 * k)
    lax.fori_loop(0, 2, step, 0)

    def columns_here(c):
        row = pl.multiple_of(8 + c * 16, 8)
        wait_columns(row, 16, c)
        unpack(ST, 3, XR, row, 16)

    def chunk(c, carry):
        @pl.when(c + COLUMNS_AHEAD < CHUNKS)
        def _():
            columns(c + COLUMNS_AHEAD)

        columns_here(c)
        inner(c).wait_recv()

        @pl.when(c + BORDERS_AHEAD < CHUNKS)
        def _():
            border(c + BORDERS_AHEAD).start()

        @pl.when(c + INNERS_AHEAD < CHUNKS - 1)
        def _():
            inner(c + INNERS_AHEAD).start()

        @pl.when(c + INNERS_AHEAD == CHUNKS - 1)
        def _():
            last_inner(0).start()
            last_inner(1).start()

        totals(range(2, 5), pl.multiple_of(8 + c * 16, 8), 16)
        lax.fori_loop(2 * c + 2, 2 * c + 4, step, 0)
        return carry

    lax.fori_loop(0, CHUNKS - 1, chunk, 0)
    columns_here(CHUNKS - 1)
    last_inner(0).wait_recv()
    totals(range(2, 5), ROWS - 24, 8)
    lax.fori_loop(30, 31, step, 0)
    last_inner(1).wait_recv()
    totals(range(2, 5), ROWS - 16, 8)
    lax.fori_loop(31, 34, step, 0)
    for t in range(34, 40):
        for lag in range(t - 33, 8):
            half_stage(lag, t + FIRST - lag)

    remote(PT, QT, cat_send, cat_recv.at[0], peer).wait_send()
    remote(XS, XR, lon_send, lon_recv.at[0], sides[0]).wait_send()
    remote(LS, LR, edge_send, edge_recv, sides[0]).wait_send()
    remote(HS, HR, halo_send, halo_recv, sides[0]).wait_send()


def shards(*arrays):
    dma = pltpu.SemaphoreType.DMA
    f32 = jnp.float32
    result = pl.pallas_call(
        kernel,
        out_shape=jax.ShapeDtypeStruct((5, ROWS, COLS), f32),
        in_specs=[pl.BlockSpec(memory_space=pltpu.HBM)] * len(arrays),
        out_specs=pl.BlockSpec(memory_space=pltpu.VMEM),
        scratch_shapes=[
            pltpu.VMEM((12, 6, HEIGHT, 128), f32),
            pltpu.SMEM((NCAT,), f32),
            pltpu.VMEM((2, NCAT, ROWS, COLS), jnp.bfloat16),
            pltpu.VMEM((ROWS, COLS), jnp.int32),
            pltpu.VMEM((ROWS, COLS), jnp.int32),
            pltpu.VMEM((3, TILES, ROWS, 128), f32),
            pltpu.VMEM((3, TILES, ROWS, 128), f32),
            pltpu.VMEM((2, ROWS, 128), f32),
            pltpu.VMEM((2, ROWS, 128), f32),
            pltpu.VMEM((2, ROWS, 128), f32),
            pltpu.VMEM((2, ROWS, 128), f32),
            pltpu.VMEM((2, 16, 128), f32),
            pltpu.VMEM((2, 16, 128), f32),
            dma,
            dma((2 * CHUNKS + 3,)),
            dma,
            dma((CHUNKS + 2,)),
            dma,
            dma,
            dma((2,)),
            dma((2,)),
            dma,
            dma,
            dma((len(LOADS),)),
            dma((len(TOPS),)),
            dma((3,)),
            pltpu.SemaphoreType.REGULAR,
        ],
        compiler_params=pltpu.CompilerParams(
            collective_id=0, has_side_effects=True, vmem_limit_bytes=44 * 2**20
        ),
        name="ice",
    )(*(pltpu.with_memory_space_constraint(a, pltpu.HBM) for a in arrays))
    return tuple(result[i] for i in range(5))


def solution(mesh):
    block = P("cat", "lat", "lon")
    plane = P("lat", "lon")
    return jax.shard_map(
        shards,
        mesh=mesh,
        in_specs=(block, block, P("cat"), *[plane] * 10),
        out_specs=(plane,) * 5,
        check_vma=False,
    )
```

```python
import jax
import jax.numpy as jnp
from jax import lax
from jax.experimental import pallas as pl
from jax.experimental.pallas import tpu as pltpu
from jax.sharding import PartitionSpec as P

U, V, S1, S2, S12, WX, WY, DR, WT, ST, MA, CO = range(12)
NCAT = 20
ROWS = 256
COLS = 640
TILES = 5
CHUNKS = 15
COLUMNS_AHEAD = 6
BORDERS_AHEAD = 12
INNERS_AHEAD = 6
ORDER = (0, 4, 1, 2, 3)
TOP_ROW = 72
HEIGHT = 344
FIRST, LAST = 8, 41
LOADS = ((0, 16), (240, 16), (16, 48), (64, 64), (128, 64), (192, 48))
TOPS = ((0, 16), (240, 16), (16, 224))
MESH = pl.DeviceIdType.MESH


def kernel(th, ar, weight, top, land, u0, v0, d0, t0, h0, wx0, wy0, dr0, out,
           F, W, TA, TOP, LAND, PT, QT, LS, LR, XS, XR, HS, HR,
           cat_send, cat_recv, lon_send, lon_recv, edge_send, edge_recv, lat_send, lat_recv, halo_send, halo_recv,
           load_sem, top_sem, field_sem, near):
    cat, lat, lon = lax.axis_index("cat"), lax.axis_index("lat"), lax.axis_index("lon")
    peer = (1 - cat, lat, lon)
    sides = ((cat, lat, lax.rem(lon + 15, 16)), (cat, lat, lax.rem(lon + 1, 16)))
    up = (cat, lax.rem(lat + 3, 4), lon)
    down = (cat, lax.rem(lat + 1, 4), lon)
    cross_up = (1 - cat, lax.rem(lat + 3, 4), lon)
    cross_down = (1 - cat, lax.rem(lat + 1, 4), lon)
    has_up, has_down = lat > 0, lat < 3

    even = lax.rem(lon, 2) == 0

    def load_rows(i):
        return pl.ds(*LOADS[i])

    def start_load(i):
        rows = load_rows(i)
        if i < len(TOPS):
            some = pl.ds(*TOPS[i])
            pltpu.make_async_copy(top.at[some, :], TOP.at[some, :], top_sem.at[i]).start()
        for k, ref in enumerate((th, ar)):
            pltpu.make_async_copy(ref.at[:, rows, :], TA.at[k, :, rows, :], load_sem.at[i]).start()

    def wait_load(i):
        if i < len(TOPS):
            some = TOP.at[pl.ds(*TOPS[i]), :]
            pltpu.make_async_copy(some, some, top_sem.at[i]).wait()
        both = TA.at[:, :, load_rows(i), :]
        pltpu.make_async_copy(both, both, load_sem.at[i]).wait()

    lands = pltpu.make_async_copy(land, LAND, field_sem.at[1])
    weights = pltpu.make_async_copy(weight, W, field_sem.at[2])

    def start_fields():
        for f, ref in enumerate((u0, v0, d0, t0, h0, wx0, wy0, dr0)):
            for j in range(TILES):
                pltpu.make_async_copy(
                    ref.at[:, pl.ds(j * 128, 128)], F.at[f, j, pl.ds(TOP_ROW, ROWS), :], field_sem.at[0]
                ).start()
        lands.start()

    def wait_fields():
        given = F.at[pl.ds(0, 8), pl.ds(0, TILES), pl.ds(TOP_ROW, ROWS), :]
        pltpu.make_async_copy(given, given, field_sem.at[0]).wait()
        lands.wait()

    start_load(0)
    weights.start()
    start_load(1)
    barrier = pltpu.get_barrier_semaphore()
    pl.semaphore_signal(barrier, inc=1, device_id=peer, device_id_type=MESH)
    inside = (lat == 1) | (lat == 2)
    for there, device in ((has_up, up), (has_down, down), (lat == 2, cross_up), (lat == 1, cross_down)):
        @pl.when(there)
        def _():
            pl.semaphore_signal(barrier, inc=1, device_id=device, device_id_type=MESH)

    @pl.when(even)
    def _():
        for device in sides:
            pl.semaphore_signal(barrier, inc=1, device_id=device, device_id_type=MESH)

    def enter():
        for middle in range(2):
            @pl.when(inside == bool(middle))
            def _():
                partners = 4 if middle else 2

                @pl.when(even)
                def _():
                    pl.semaphore_wait(barrier, partners)

                @pl.when(jnp.logical_not(even))
                def _():
                    pl.semaphore_wait(barrier, partners + 2)

        @pl.when(jnp.logical_not(even))
        def _():
            for device in sides:
                pl.semaphore_signal(near, inc=1, device_id=device, device_id_type=MESH)

    start_load(2)
    start_load(3)

    @pl.when(lat == 0)
    def _():
        F[:, :, pl.ds(8 * FIRST, 8), :] = jnp.zeros((12, 6, 8, 128), jnp.float32)

    @pl.when(lat == 3)
    def _():
        F[:, :, pl.ds(8 * LAST, 8), :] = jnp.zeros((12, 6, 8, 128), jnp.float32)

    lane = lax.broadcasted_iota(jnp.int32, (8, 128), 1)
    lane16 = lax.broadcasted_iota(jnp.int32, (16, 128), 1)
    base = cat * NCAT

    def sums(block, carry):
        rows = pl.ds(pl.multiple_of(block * 16, 16), 16)
        for place, j in enumerate(ORDER):
            cols = pl.ds(j * 128, 128)
            limit = TOP[rows, cols] - base
            strength = jnp.zeros((16, 128), jnp.float32)
            mass = jnp.zeros((16, 128), jnp.float32)
            cover = jnp.zeros((16, 128), jnp.float32)
            for n in range(NCAT):
                h = TA[0, n, rows, cols].astype(jnp.float32)
                c = TA[1, n, rows, cols].astype(jnp.float32)
                c = jnp.where(limit > n, c, 0.0)
                m = c * h
                cover = cover + c
                mass = mass + m
                strength = strength + (W[n] * h) * m
            PT[0, place, rows, :] = strength
            PT[1, place, rows, :] = mass
            PT[2, place, rows, :] = cover
        return carry

    def remote(src, dst, send, recv, device):
        return pltpu.make_async_remote_copy(
            src_ref=src, dst_ref=dst, send_sem=send, recv_sem=recv, device_id=device, device_id_type=MESH
        )

    def cat_message(tiles, rows, k):
        where = (slice(None), tiles, rows, slice(None))
        return remote(PT.at[where], QT.at[where], cat_send, cat_recv.at[k], peer)

    def sixteen(c):
        return pl.ds(pl.multiple_of(8 + c * 16, 8), 16)

    def border(c):
        first = isinstance(c, int) and c < COLUMNS_AHEAD
        return cat_message(pl.ds(0, 2), sixteen(c), CHUNKS + 1 + c // 3 if first else c - COLUMNS_AHEAD)

    def inner(c):
        return cat_message(pl.ds(2, 3), sixteen(c), c)

    def last_inner(k):
        return cat_message(pl.ds(2, 3), pl.ds(ROWS - 24 + 8 * k, 8), CHUNKS - 1 + k)

    def edge(k):
        return cat_message(pl.ds(0, 5), pl.ds(248 * k, 8), CHUNKS + 3)

    def wait_first_borders(group):
        cat_message(pl.ds(0, 2), pl.ds(8, 48), CHUNKS + 1 + group).wait_recv()

    def wait_edges():
        cat_message(pl.ds(0, 5), pl.ds(0, 16), CHUNKS + 3).wait_recv()

    def wait_both(c):
        cat_message(pl.ds(0, 5), sixteen(c), c).wait_recv()

    def start_columns(start, size, k):
        rows = pl.ds(start, size)
        for d in range(2):
            remote(XS.at[d, rows, :], XR.at[d, rows, :], lon_send, lon_recv.at[k], sides[d]).start()

    def wait_columns(start, size, k):
        rows = pl.ds(start, size)
        remote(XS.at[:, rows, :], XR.at[:, rows, :], lon_send, lon_recv.at[k], sides[0]).wait_recv()

    def lat_copy(d, fields, tiles, over=False):
        here, there, device = ((FIRST + 1, LAST, (up, cross_up)[over]), (LAST - 1, FIRST, (down, cross_down)[over]))[d]
        return remote(
            F.at[fields, tiles, pl.ds(8 * here, 8), :], F.at[fields, tiles, pl.ds(8 * there, 8), :],
            lat_send.at[d], lat_recv.at[d], device,
        )

    def to_rows(k):
        fields = (pl.ds(0, 9), pl.ds(9, 3))[k]
        halves = (
            (((pl.ds(0, 9), pl.ds(0, 2)), (pl.ds(0, 6), pl.ds(2, 1))), ((pl.ds(0, 9), pl.ds(3, 2)), (pl.ds(6, 3), pl.ds(2, 1)))),
            (((pl.ds(9, 3), pl.ds(0, 2)),), ((pl.ds(9, 3), pl.ds(2, 3)),)),
        )[k]
        for d in range(2):
            crosses = lat == (2, 1)[d]

            @pl.when((has_up, has_down)[d] & jnp.logical_not(crosses))
            def _():
                lat_copy(d, fields, pl.ds(0, TILES)).start()

            for holder in range(2):
                @pl.when(crosses & (cat == holder))
                def _():
                    for some, tiles in halves[holder]:
                        for over in range(2):
                            lat_copy(d, some, tiles, over).start()

    def pack(first, count, send, row, size, place=None):
        iota = lane if size == 8 else lane16
        rows = pl.ds(row if place is None else place, size)
        from_rows = pl.ds(row + TOP_ROW, size)
        left = jnp.zeros((size, 128), jnp.float32)
        right = jnp.zeros((size, 128), jnp.float32)
        for i in range(count):
            mine = (iota >= 8 * i) & (iota < 8 * i + 8)
            a = F[first + i, 0, from_rows, :]
            b = F[first + i, 4, from_rows, :]
            left = jnp.where(mine, pltpu.roll(a, 8 * i, 1) if i else a, left)
            right = jnp.where(mine, pltpu.roll(b, 8 * i + 8, 1), right)
        send[0, rows, :] = left
        send[1, rows, :] = right

    def unpack(first, count, recv, row, size, place=None):
        iota = lane if size == 8 else lane16
        rows = pl.ds(row if place is None else place, size)
        a = recv[0, rows, :]
        b = recv[1, rows, :]
        for i in range(count):
            ahead = pltpu.roll(a, 128 - 8 * i, 1) if i else a
            behind = pltpu.roll(b, 120 - 8 * i, 1)
            F[first + i, 5, pl.ds(row + TOP_ROW, size), :] = jnp.where(
                iota < 8, ahead, jnp.where(iota >= 120, behind, 0.0)
            )

    def totals(places, row, size):
        for place in places:
            for f in range(3):
                F[ST + f, ORDER[place], pl.ds(row + TOP_ROW, size), :] = (
                    PT[f, place, pl.ds(row, size), :] + QT[f, place, pl.ds(row, size), :]
                )

    def right_less_left(before, here, after):
        ahead = pltpu.roll(jnp.where(lane == 0, after, here), 127, 1)
        behind = pltpu.roll(jnp.where(lane == 127, before, here), 1, 1)
        return ahead - behind

    def coefficients(band):
        rows = pl.ds(pl.multiple_of(8 * band, 8), 8)
        for j in range(6):
            wet = F[WT, j, rows, :]
            mass = F[MA, j, rows, :]
            cover = F[CO, j, rows, :]
            g = wet / (mass + F[DR, j, rows, :] + 1.0 - wet)
            push = g * cover
            F[MA, j, rows, :] = g * mass
            F[WX, j, rows, :] = push * F[WX, j, rows, :]
            F[WY, j, rows, :] = push * F[WY, j, rows, :]
            F[DR, j, rows, :] = 0.25 * g
            F[WT, j, rows, :] = wet * (1.0 / 3.0)
            F[ST, j, rows, :] = (wet * (2.0 / 3.0)) * F[ST, j, rows, :]

    def stress(band, last=None):
        row = pl.multiple_of(8 * band, 8)
        rows, above, below = pl.ds(row, 8), pl.ds(row - 1, 8), pl.ds(row + 1, 8)
        for j in range(6):
            before, after = (j + 5) % 6, (j + 1) % 6
            ux = right_less_left(F[U, before, rows, :], F[U, j, rows, :], F[U, after, rows, :])
            vx = right_less_left(F[V, before, rows, :], F[V, j, rows, :], F[V, after, rows, :])
            uy = F[U, j, below, :] - F[U, j, above, :]
            vy = F[V, j, below, :] - F[V, j, above, :]
            div, ten, shr = ux + vy, ux - vy, uy + vx
            square = div * div + 0.25 * (ten * ten + shr * shr) + 0.01
            strength = F[ST, j, rows, :]
            half = strength * lax.rsqrt(square)
            eighth = 0.25 * half
            third = F[WT, j, rows, :]
            s1 = third * F[S1, j, rows, :] + (half * div - strength)
            s2 = third * F[S2, j, rows, :] + eighth * ten
            s12 = third * F[S12, j, rows, :] + eighth * shr
            F[S1, j, rows, :] = s1
            F[S2, j, rows, :] = s2
            F[S12, j, rows, :] = s12
            if last is not None and j < TILES:
                place = (pl.ds(last, 8), pl.ds(j * 128, 128))
                out[(S1, *place)] = s1
                out[(S2, *place)] = s2
                out[(S12, *place)] = s12

    def momentum(band, last=None):
        row = pl.multiple_of(8 * band, 8)
        rows, above, below = pl.ds(row, 8), pl.ds(row - 1, 8), pl.ds(row + 1, 8)
        for j in range(6):
            around = ((j + 5) % 6, j, (j + 1) % 6)
            px = right_less_left(*(F[S1, k, rows, :] + F[S2, k, rows, :] for k in around))
            cx = right_less_left(*(F[S12, k, rows, :] for k in around))
            cy = F[S12, j, below, :] - F[S12, j, above, :]
            my = (F[S1, j, below, :] - F[S2, j, below, :]) - (F[S1, j, above, :] - F[S2, j, above, :])
            a, g = F[MA, j, rows, :], F[DR, j, rows, :]
            u, v = F[U, j, rows, :], F[V, j, rows, :]
            next_u = a * (u + 0.5 * v) + g * (px + 2.0 * cy) + F[WX, j, rows, :]
            next_v = a * (v - 0.5 * u) + g * (2.0 * cx + my) + F[WY, j, rows, :]
            if last is None:
                F[U, j, rows, :] = next_u
                F[V, j, rows, :] = next_v
            elif j < TILES:
                place = (pl.ds(last, 8), pl.ds(j * 128, 128))
                out[(U, *place)] = next_u
                out[(V, *place)] = next_v

    def half_stage(lag, band):
        last = None
        if lag >= 6:
            row = 8 * (band - FIRST - 1)
            last = max(row, 0) if isinstance(band, int) else pl.multiple_of(jnp.maximum(row, 0), 8)
            if isinstance(band, int) and band == LAST:
                last = None
        (momentum if lag % 2 else stress)(band, last)

    def step(t, carry):
        coefficients(t + FIRST)
        for lag in range(8):
            half_stage(lag, t + (FIRST - lag))
        return carry

    weights.wait()
    wait_load(0)
    sums(0, 0)
    enter()
    edge(0).start()
    start_fields()
    start_load(4)
    start_load(5)
    wait_load(1)
    sums(15, 0)
    edge(1).start()
    wait_load(2)
    lax.fori_loop(1, 4, sums, 0)
    for c in range(3):
        border(c).start()
    inner(0).start()
    wait_load(3)
    lax.fori_loop(4, 8, sums, 0)
    border(3).start()
    border(4).start()

    wait_fields()

    def given(block, carry):
        row = pl.multiple_of(block * 16, 16)
        for j in range(TILES):
            F[WT, j, pl.ds(row + TOP_ROW, 16), :] = LAND[pl.ds(row, 16), pl.ds(j * 128, 128)].astype(jnp.float32)
        pack(0, 9, LS, row, 16)
        return carry

    lax.fori_loop(0, 16, given, 0)

    @pl.when(even)
    def _():
        pl.semaphore_wait(near, 2)

    for d in range(2):
        remote(LS.at[d], LR.at[d], edge_send, edge_recv, sides[d]).start()

    to_rows(0)

    wait_edges()
    for k in range(2):
        totals(range(5), 248 * k, 8)
        pack(ST, 3, XS, 248 * k, 8)
        start_columns(248 * k, 8, CHUNKS)
    to_rows(1)
    inner(1).start()
    border(5).start()
    wait_load(4)
    wait_load(5)
    lax.fori_loop(8, 15, sums, 0)

    for c in range(3):
        border(2 * c + 6).start()
        border(2 * c + 7).start()
        inner(c + 2).start()
    inner(5).start()
    remote(LS, LR, edge_send, edge_recv, sides[0]).wait_recv()

    def take(block, carry):
        unpack(0, 9, LR, pl.multiple_of(block * 16, 16), 16)
        return carry

    lax.fori_loop(0, 16, take, 0)
    wait_columns(0, 16, CHUNKS)
    for k in range(2):
        unpack(ST, 3, XR, 248 * k, 8)

    def columns(c):
        row = pl.multiple_of(8 + c * 16, 8)
        totals(range(2), row, 16)
        pack(ST, 3, XS, row, 16)
        start_columns(row, 16, c)

    wait_first_borders(0)
    for c in range(3):
        columns(c)
    halo = (slice(None), pl.ds(0, TILES))

    @pl.when(has_down)
    def _():
        lat_copy(0, *halo).wait_recv()
        lat_copy(1, *halo).wait_send()

    @pl.when(has_up)
    def _():
        lat_copy(1, *halo).wait_recv()
        lat_copy(0, *halo).wait_send()

    for k in range(2):
        pack(0, 12, HS, (-8, ROWS)[k], 8, 8 * k)
    for d in range(2):
        remote(HS.at[d], HR.at[d], halo_send, halo_recv, sides[d]).start()
    wait_first_borders(1)
    for c in range(3, COLUMNS_AHEAD):
        columns(c)
    remote(HS, HR, halo_send, halo_recv, sides[0]).wait_recv()
    for k in range(2):
        unpack(0, 12, HR, (-8, ROWS)[k], 8, 8 * k)
    lax.fori_loop(0, 2, step, 0)

    def columns_here(c):
        row = pl.multiple_of(8 + c * 16, 8)
        wait_columns(row, 16, c)
        unpack(ST, 3, XR, row, 16)

    def chunk(c, carry):
        @pl.when(c + COLUMNS_AHEAD < CHUNKS)
        def _():
            wait_both(c)
            columns(c + COLUMNS_AHEAD)

        @pl.when(c + COLUMNS_AHEAD >= CHUNKS)
        def _():
            inner(c).wait_recv()

        columns_here(c)

        @pl.when(c + BORDERS_AHEAD < CHUNKS)
        def _():
            border(c + BORDERS_AHEAD).start()

        @pl.when(c + INNERS_AHEAD < CHUNKS - 1)
        def _():
            inner(c + INNERS_AHEAD).start()

        @pl.when(c + INNERS_AHEAD == CHUNKS - 1)
        def _():
            last_inner(0).start()
            last_inner(1).start()

        totals(range(2, 5), pl.multiple_of(8 + c * 16, 8), 16)
        lax.fori_loop(2 * c + 2, 2 * c + 4, step, 0)
        return carry

    lax.fori_loop(0, CHUNKS - 1, chunk, 0)
    columns_here(CHUNKS - 1)
    last_inner(0).wait_recv()
    totals(range(2, 5), ROWS - 24, 8)
    lax.fori_loop(30, 31, step, 0)
    for band in (LAST - 1, LAST):
        coefficients(band)
        half_stage(0, band)
    half_stage(1, LAST)
    last_inner(1).wait_recv()
    totals(range(2, 5), ROWS - 16, 8)
    lax.fori_loop(31, 32, step, 0)
    for t in range(32, 40):
        for lag in range(max(1, t - 33), 8):
            if (t, lag) != (34, 1):
                half_stage(lag, t + FIRST - lag)

    remote(PT, QT, cat_send, cat_recv.at[0], peer).wait_send()
    remote(XS, XR, lon_send, lon_recv.at[0], sides[0]).wait_send()
    remote(LS, LR, edge_send, edge_recv, sides[0]).wait_send()
    remote(HS, HR, halo_send, halo_recv, sides[0]).wait_send()


def shards(*arrays):
    dma = pltpu.SemaphoreType.DMA
    f32 = jnp.float32
    result = pl.pallas_call(
        kernel,
        out_shape=jax.ShapeDtypeStruct((5, ROWS, COLS), f32),
        in_specs=[pl.BlockSpec(memory_space=pltpu.HBM)] * len(arrays),
        out_specs=pl.BlockSpec(memory_space=pltpu.VMEM),
        scratch_shapes=[
            pltpu.VMEM((12, 6, HEIGHT, 128), f32),
            pltpu.SMEM((NCAT,), f32),
            pltpu.VMEM((2, NCAT, ROWS, COLS), jnp.bfloat16),
            pltpu.VMEM((ROWS, COLS), jnp.int32),
            pltpu.VMEM((ROWS, COLS), jnp.int32),
            pltpu.VMEM((3, TILES, ROWS, 128), f32),
            pltpu.VMEM((3, TILES, ROWS, 128), f32),
            pltpu.VMEM((2, ROWS, 128), f32),
            pltpu.VMEM((2, ROWS, 128), f32),
            pltpu.VMEM((2, ROWS, 128), f32),
            pltpu.VMEM((2, ROWS, 128), f32),
            pltpu.VMEM((2, 16, 128), f32),
            pltpu.VMEM((2, 16, 128), f32),
            dma,
            dma((CHUNKS + 4,)),
            dma,
            dma((CHUNKS + 1,)),
            dma,
            dma,
            dma((2,)),
            dma((2,)),
            dma,
            dma,
            dma((len(LOADS),)),
            dma((len(TOPS),)),
            dma((3,)),
            pltpu.SemaphoreType.REGULAR,
        ],
        compiler_params=pltpu.CompilerParams(
            collective_id=0, has_side_effects=True, vmem_limit_bytes=44 * 2**20
        ),
        name="ice",
    )(*(pltpu.with_memory_space_constraint(a, pltpu.HBM) for a in arrays))
    return tuple(result[i] for i in range(5))


def solution(mesh):
    block = P("cat", "lat", "lon")
    plane = P("lat", "lon")
    return jax.shard_map(
        shards,
        mesh=mesh,
        in_specs=(block, block, P("cat"), *[plane] * 10),
        out_specs=(plane,) * 5,
        check_vma=False,
    )
```

```python
import jax
import jax.numpy as jnp
from jax import lax
from jax.experimental import pallas as pl
from jax.experimental.pallas import tpu as pltpu
from jax.sharding import PartitionSpec as P

U, V, S1, S2, S12, WX, WY, DR, WT, ST, MA, CO = range(12)
NCAT = 20
ROWS = 256
COLS = 640
TILES = 5
CHUNKS = 15
COLUMNS_AHEAD = 6
BORDERS_AHEAD = 12
INNERS_AHEAD = 6
ORDER = (0, 4, 1, 2, 3)
TOP_ROW = 72
HEIGHT = 344
FIRST, LAST = 8, 41
LOADS = ((0, 16), (240, 16), (16, 48), (64, 64), (128, 64), (192, 48))
TOPS = ((0, 16), (240, 16), (16, 224))
MESH = pl.DeviceIdType.MESH


def kernel(th, ar, weight, top, land, u0, v0, d0, t0, h0, wx0, wy0, dr0, out,
           F, W, TA, TOP, LAND, PT, QT, LS, LR, XS, XR, HS, HR,
           cat_send, cat_recv, lon_send, lon_recv, edge_send, edge_recv, lat_send, lat_recv, halo_send, halo_recv,
           load_sem, top_sem, field_sem, near):
    cat, lat, lon = lax.axis_index("cat"), lax.axis_index("lat"), lax.axis_index("lon")
    peer = (1 - cat, lat, lon)
    sides = ((cat, lat, lax.rem(lon + 15, 16)), (cat, lat, lax.rem(lon + 1, 16)))
    up = (cat, lax.rem(lat + 3, 4), lon)
    down = (cat, lax.rem(lat + 1, 4), lon)
    cross_up = (1 - cat, lax.rem(lat + 3, 4), lon)
    cross_down = (1 - cat, lax.rem(lat + 1, 4), lon)
    has_up, has_down = lat > 0, lat < 3

    even = lax.rem(lon, 2) == 0

    def load_rows(i):
        return pl.ds(*LOADS[i])

    def start_load(i):
        rows = load_rows(i)
        if i < len(TOPS):
            some = pl.ds(*TOPS[i])
            pltpu.make_async_copy(top.at[some, :], TOP.at[some, :], top_sem.at[i]).start()
        for k, ref in enumerate((th, ar)):
            pltpu.make_async_copy(ref.at[:, rows, :], TA.at[k, :, rows, :], load_sem.at[i]).start()

    def wait_load(i):
        if i < len(TOPS):
            some = TOP.at[pl.ds(*TOPS[i]), :]
            pltpu.make_async_copy(some, some, top_sem.at[i]).wait()
        both = TA.at[:, :, load_rows(i), :]
        pltpu.make_async_copy(both, both, load_sem.at[i]).wait()

    lands = pltpu.make_async_copy(land, LAND, field_sem.at[1])
    weights = pltpu.make_async_copy(weight, W, field_sem.at[2])

    def start_fields():
        for f, ref in enumerate((u0, v0, d0, t0, h0, wx0, wy0, dr0)):
            for j in range(TILES):
                pltpu.make_async_copy(
                    ref.at[:, pl.ds(j * 128, 128)], F.at[f, j, pl.ds(TOP_ROW, ROWS), :], field_sem.at[0]
                ).start()
        lands.start()

    def wait_fields():
        given = F.at[pl.ds(0, 8), pl.ds(0, TILES), pl.ds(TOP_ROW, ROWS), :]
        pltpu.make_async_copy(given, given, field_sem.at[0]).wait()
        lands.wait()

    start_load(0)
    weights.start()
    start_load(1)
    barrier = pltpu.get_barrier_semaphore()
    pl.semaphore_signal(barrier, inc=1, device_id=peer, device_id_type=MESH)
    inside = (lat == 1) | (lat == 2)
    for there, device in ((has_up, up), (has_down, down), (lat == 2, cross_up), (lat == 1, cross_down)):
        @pl.when(there)
        def _():
            pl.semaphore_signal(barrier, inc=1, device_id=device, device_id_type=MESH)

    @pl.when(even)
    def _():
        for device in sides:
            pl.semaphore_signal(barrier, inc=1, device_id=device, device_id_type=MESH)

    def enter():
        for middle in range(2):
            @pl.when(inside == bool(middle))
            def _():
                partners = 4 if middle else 2

                @pl.when(even)
                def _():
                    pl.semaphore_wait(barrier, partners)

                @pl.when(jnp.logical_not(even))
                def _():
                    pl.semaphore_wait(barrier, partners + 2)

        @pl.when(jnp.logical_not(even))
        def _():
            for device in sides:
                pl.semaphore_signal(near, inc=1, device_id=device, device_id_type=MESH)

    start_load(2)
    start_load(3)

    @pl.when(lat == 0)
    def _():
        F[:, :, pl.ds(8 * FIRST, 8), :] = jnp.zeros((12, 6, 8, 128), jnp.float32)

    @pl.when(lat == 3)
    def _():
        F[:, :, pl.ds(8 * LAST, 8), :] = jnp.zeros((12, 6, 8, 128), jnp.float32)

    lane = lax.broadcasted_iota(jnp.int32, (8, 128), 1)
    lane16 = lax.broadcasted_iota(jnp.int32, (16, 128), 1)
    base = cat * NCAT

    def sums(block, carry):
        rows = pl.ds(pl.multiple_of(block * 16, 16), 16)
        for place, j in enumerate(ORDER):
            cols = pl.ds(j * 128, 128)
            limit = TOP[rows, cols] - base
            strength = jnp.zeros((16, 128), jnp.float32)
            mass = jnp.zeros((16, 128), jnp.float32)
            cover = jnp.zeros((16, 128), jnp.float32)
            for n in range(NCAT):
                h = TA[0, n, rows, cols].astype(jnp.float32)
                c = TA[1, n, rows, cols].astype(jnp.float32)
                c = jnp.where(limit > n, c, 0.0)
                m = c * h
                cover = cover + c
                mass = mass + m
                strength = strength + (W[n] * h) * m
            PT[0, place, rows, :] = strength
            PT[1, place, rows, :] = mass
            PT[2, place, rows, :] = cover
        return carry

    def remote(src, dst, send, recv, device):
        return pltpu.make_async_remote_copy(
            src_ref=src, dst_ref=dst, send_sem=send, recv_sem=recv, device_id=device, device_id_type=MESH
        )

    def cat_message(tiles, rows, k):
        where = (slice(None), tiles, rows, slice(None))
        return remote(PT.at[where], QT.at[where], cat_send, cat_recv.at[k], peer)

    def sixteen(c):
        return pl.ds(pl.multiple_of(8 + c * 16, 8), 16)

    def border(c):
        first = isinstance(c, int) and c < COLUMNS_AHEAD
        return cat_message(pl.ds(0, 2), sixteen(c), CHUNKS + 1 + c // 3 if first else c - COLUMNS_AHEAD)

    def inner(c):
        return cat_message(pl.ds(2, 3), sixteen(c), c)

    def last_inner(k):
        return cat_message(pl.ds(2, 3), pl.ds(ROWS - 24 + 8 * k, 8), CHUNKS - 1 + k)

    def edge(k):
        return cat_message(pl.ds(0, 5), pl.ds(248 * k, 8), CHUNKS + 3)

    def wait_first_borders(group):
        cat_message(pl.ds(0, 2), pl.ds(8, 48), CHUNKS + 1 + group).wait_recv()

    def wait_edges():
        cat_message(pl.ds(0, 5), pl.ds(0, 16), CHUNKS + 3).wait_recv()

    def wait_both(c):
        cat_message(pl.ds(0, 5), sixteen(c), c).wait_recv()

    def start_columns(start, size, k):
        rows = pl.ds(start, size)
        for d in range(2):
            remote(XS.at[d, rows, :], XR.at[d, rows, :], lon_send, lon_recv.at[k], sides[d]).start()

    def wait_columns(start, size, k):
        rows = pl.ds(start, size)
        remote(XS.at[:, rows, :], XR.at[:, rows, :], lon_send, lon_recv.at[k], sides[0]).wait_recv()

    def lat_copy(d, fields, tiles, over=False):
        here, there, device = ((FIRST + 1, LAST, (up, cross_up)[over]), (LAST - 1, FIRST, (down, cross_down)[over]))[d]
        return remote(
            F.at[fields, tiles, pl.ds(8 * here, 8), :], F.at[fields, tiles, pl.ds(8 * there, 8), :],
            lat_send.at[d], lat_recv.at[d], device,
        )

    def to_rows(k):
        fields = (pl.ds(0, 9), pl.ds(9, 3))[k]
        halves = (
            (((pl.ds(0, 9), pl.ds(0, 2)), (pl.ds(0, 6), pl.ds(2, 1))), ((pl.ds(0, 9), pl.ds(3, 2)), (pl.ds(6, 3), pl.ds(2, 1)))),
            (((pl.ds(9, 3), pl.ds(0, 2)),), ((pl.ds(9, 3), pl.ds(2, 3)),)),
        )[k]
        for d in range(2):
            crosses = lat == (2, 1)[d]

            @pl.when((has_up, has_down)[d] & jnp.logical_not(crosses))
            def _():
                lat_copy(d, fields, pl.ds(0, TILES)).start()

            for holder in range(2):
                @pl.when(crosses & (cat == holder))
                def _():
                    for some, tiles in halves[holder]:
                        for over in range(2):
                            lat_copy(d, some, tiles, over).start()

    def pack(first, count, send, row, size, place=None):
        iota = lane if size == 8 else lane16
        rows = pl.ds(row if place is None else place, size)
        from_rows = pl.ds(row + TOP_ROW, size)
        left = jnp.zeros((size, 128), jnp.float32)
        right = jnp.zeros((size, 128), jnp.float32)
        for i in range(count):
            mine = (iota >= 8 * i) & (iota < 8 * i + 8)
            a = F[first + i, 0, from_rows, :]
            b = F[first + i, 4, from_rows, :]
            left = jnp.where(mine, pltpu.roll(a, 8 * i, 1) if i else a, left)
            right = jnp.where(mine, pltpu.roll(b, 8 * i + 8, 1), right)
        send[0, rows, :] = left
        send[1, rows, :] = right

    def unpack(first, count, recv, row, size, place=None):
        iota = lane if size == 8 else lane16
        rows = pl.ds(row if place is None else place, size)
        a = recv[0, rows, :]
        b = recv[1, rows, :]
        for i in range(count):
            ahead = pltpu.roll(a, 128 - 8 * i, 1) if i else a
            behind = pltpu.roll(b, 120 - 8 * i, 1)
            F[first + i, 5, pl.ds(row + TOP_ROW, size), :] = jnp.where(
                iota < 8, ahead, jnp.where(iota >= 120, behind, 0.0)
            )

    def totals(places, row, size):
        for place in places:
            for f in range(3):
                F[ST + f, ORDER[place], pl.ds(row + TOP_ROW, size), :] = (
                    PT[f, place, pl.ds(row, size), :] + QT[f, place, pl.ds(row, size), :]
                )

    def right_less_left(before, here, after):
        ahead = pltpu.roll(jnp.where(lane == 0, after, here), 127, 1)
        behind = pltpu.roll(jnp.where(lane == 127, before, here), 1, 1)
        return ahead - behind

    def coefficients(band):
        rows = pl.ds(pl.multiple_of(8 * band, 8), 8)
        for j in range(6):
            wet = F[WT, j, rows, :]
            mass = F[MA, j, rows, :]
            cover = F[CO, j, rows, :]
            g = wet / (mass + F[DR, j, rows, :] + 1.0 - wet)
            push = g * cover
            F[MA, j, rows, :] = g * mass
            F[WX, j, rows, :] = push * F[WX, j, rows, :]
            F[WY, j, rows, :] = push * F[WY, j, rows, :]
            F[DR, j, rows, :] = 0.25 * g
            F[WT, j, rows, :] = wet * (1.0 / 3.0)
            F[ST, j, rows, :] = (wet * (2.0 / 3.0)) * F[ST, j, rows, :]

    def stress(band, last=None):
        row = pl.multiple_of(8 * band, 8)
        rows, above, below = pl.ds(row, 8), pl.ds(row - 1, 8), pl.ds(row + 1, 8)
        for j in range(6):
            before, after = (j + 5) % 6, (j + 1) % 6
            ux = right_less_left(F[U, before, rows, :], F[U, j, rows, :], F[U, after, rows, :])
            vx = right_less_left(F[V, before, rows, :], F[V, j, rows, :], F[V, after, rows, :])
            uy = F[U, j, below, :] - F[U, j, above, :]
            vy = F[V, j, below, :] - F[V, j, above, :]
            div, ten, shr = ux + vy, ux - vy, uy + vx
            square = div * div + 0.25 * (ten * ten + shr * shr) + 0.01
            strength = F[ST, j, rows, :]
            half = strength * lax.rsqrt(square)
            eighth = 0.25 * half
            third = F[WT, j, rows, :]
            s1 = third * F[S1, j, rows, :] + (half * div - strength)
            s2 = third * F[S2, j, rows, :] + eighth * ten
            s12 = third * F[S12, j, rows, :] + eighth * shr
            F[S1, j, rows, :] = s1
            F[S2, j, rows, :] = s2
            F[S12, j, rows, :] = s12
            if last is not None and j < TILES:
                place = (pl.ds(last, 8), pl.ds(j * 128, 128))
                out[(S1, *place)] = s1
                out[(S2, *place)] = s2
                out[(S12, *place)] = s12

    def momentum(band, last=None):
        row = pl.multiple_of(8 * band, 8)
        rows, above, below = pl.ds(row, 8), pl.ds(row - 1, 8), pl.ds(row + 1, 8)
        for j in range(6):
            around = ((j + 5) % 6, j, (j + 1) % 6)
            px = right_less_left(*(F[S1, k, rows, :] + F[S2, k, rows, :] for k in around))
            cx = right_less_left(*(F[S12, k, rows, :] for k in around))
            cy = F[S12, j, below, :] - F[S12, j, above, :]
            my = (F[S1, j, below, :] - F[S2, j, below, :]) - (F[S1, j, above, :] - F[S2, j, above, :])
            a, g = F[MA, j, rows, :], F[DR, j, rows, :]
            u, v = F[U, j, rows, :], F[V, j, rows, :]
            next_u = a * (u + 0.5 * v) + g * (px + 2.0 * cy) + F[WX, j, rows, :]
            next_v = a * (v - 0.5 * u) + g * (2.0 * cx + my) + F[WY, j, rows, :]
            if last is None:
                F[U, j, rows, :] = next_u
                F[V, j, rows, :] = next_v
            elif j < TILES:
                place = (pl.ds(last, 8), pl.ds(j * 128, 128))
                out[(U, *place)] = next_u
                out[(V, *place)] = next_v

    def half_stage(lag, band):
        last = None
        if lag >= 6:
            row = 8 * (band - FIRST - 1)
            last = max(row, 0) if isinstance(band, int) else pl.multiple_of(jnp.maximum(row, 0), 8)
            if isinstance(band, int) and band == LAST:
                last = None
        (momentum if lag % 2 else stress)(band, last)

    def step(t, carry):
        coefficients(t + FIRST)
        for lag in range(8):
            half_stage(lag, t + (FIRST - lag))
        return carry

    weights.wait()
    wait_load(0)
    sums(0, 0)
    enter()
    edge(0).start()
    start_fields()
    start_load(4)
    start_load(5)
    wait_load(1)
    sums(15, 0)
    edge(1).start()
    wait_load(2)
    lax.fori_loop(1, 4, sums, 0)
    for c in range(3):
        border(c).start()
    inner(0).start()
    wait_load(3)
    lax.fori_loop(4, 8, sums, 0)
    border(3).start()
    border(4).start()

    wait_fields()

    def given(block, carry):
        row = pl.multiple_of(block * 16, 16)
        for j in range(TILES):
            F[WT, j, pl.ds(row + TOP_ROW, 16), :] = LAND[pl.ds(row, 16), pl.ds(j * 128, 128)].astype(jnp.float32)
        pack(0, 9, LS, row, 16)
        return carry

    lax.fori_loop(0, 16, given, 0)

    @pl.when(even)
    def _():
        pl.semaphore_wait(near, 2)

    for d in range(2):
        remote(LS.at[d], LR.at[d], edge_send, edge_recv, sides[d]).start()

    to_rows(0)

    wait_edges()
    for k in range(2):
        totals(range(5), 248 * k, 8)
        pack(ST, 3, XS, 248 * k, 8)
        start_columns(248 * k, 8, CHUNKS)
    to_rows(1)

    @pl.when(inside)
    def _():
        inner(1).start()
        border(5).start()

    wait_load(4)
    wait_load(5)
    lax.fori_loop(8, 15, sums, 0)


    @pl.when(jnp.logical_not(inside))
    def _():
        pl.delay(1700)
        inner(1).start()
        border(5).start()

    for c in range(3):
        border(2 * c + 6).start()
        border(2 * c + 7).start()
        inner(c + 2).start()
    inner(5).start()
    remote(LS, LR, edge_send, edge_recv, sides[0]).wait_recv()

    def take(block, carry):
        unpack(0, 9, LR, pl.multiple_of(block * 16, 16), 16)
        return carry

    lax.fori_loop(0, 16, take, 0)
    wait_columns(0, 16, CHUNKS)
    for k in range(2):
        unpack(ST, 3, XR, 248 * k, 8)

    def columns(c):
        row = pl.multiple_of(8 + c * 16, 8)
        totals(range(2), row, 16)
        pack(ST, 3, XS, row, 16)
        start_columns(row, 16, c)

    wait_first_borders(0)
    for c in range(3):
        columns(c)
    halo = (slice(None), pl.ds(0, TILES))

    @pl.when(has_down)
    def _():
        lat_copy(0, *halo).wait_recv()
        lat_copy(1, *halo).wait_send()

    @pl.when(has_up)
    def _():
        lat_copy(1, *halo).wait_recv()
        lat_copy(0, *halo).wait_send()

    for k in range(2):
        pack(0, 12, HS, (-8, ROWS)[k], 8, 8 * k)
    for d in range(2):
        remote(HS.at[d], HR.at[d], halo_send, halo_recv, sides[d]).start()
    wait_first_borders(1)
    for c in range(3, COLUMNS_AHEAD):
        columns(c)
    remote(HS, HR, halo_send, halo_recv, sides[0]).wait_recv()
    for k in range(2):
        unpack(0, 12, HR, (-8, ROWS)[k], 8, 8 * k)
    lax.fori_loop(0, 2, step, 0)

    def columns_here(c):
        row = pl.multiple_of(8 + c * 16, 8)
        wait_columns(row, 16, c)
        unpack(ST, 3, XR, row, 16)

    def chunk(c, carry):
        @pl.when(c + COLUMNS_AHEAD < CHUNKS)
        def _():
            wait_both(c)
            columns(c + COLUMNS_AHEAD)

        @pl.when(c + COLUMNS_AHEAD >= CHUNKS)
        def _():
            inner(c).wait_recv()

        columns_here(c)

        @pl.when(c + BORDERS_AHEAD < CHUNKS)
        def _():
            border(c + BORDERS_AHEAD).start()

        @pl.when(c + INNERS_AHEAD < CHUNKS - 1)
        def _():
            inner(c + INNERS_AHEAD).start()

        @pl.when(c + INNERS_AHEAD == CHUNKS - 1)
        def _():
            last_inner(0).start()
            last_inner(1).start()

        totals(range(2, 5), pl.multiple_of(8 + c * 16, 8), 16)
        lax.fori_loop(2 * c + 2, 2 * c + 4, step, 0)
        return carry

    lax.fori_loop(0, CHUNKS - 1, chunk, 0)
    columns_here(CHUNKS - 1)
    last_inner(0).wait_recv()
    totals(range(2, 5), ROWS - 24, 8)
    lax.fori_loop(30, 31, step, 0)
    for band in (LAST - 1, LAST):
        coefficients(band)
        half_stage(0, band)
    half_stage(1, LAST)
    last_inner(1).wait_recv()
    totals(range(2, 5), ROWS - 16, 8)
    lax.fori_loop(31, 32, step, 0)
    for t in range(32, 40):
        for lag in range(max(1, t - 33), 8):
            if (t, lag) != (34, 1):
                half_stage(lag, t + FIRST - lag)

    remote(PT, QT, cat_send, cat_recv.at[0], peer).wait_send()
    remote(XS, XR, lon_send, lon_recv.at[0], sides[0]).wait_send()
    remote(LS, LR, edge_send, edge_recv, sides[0]).wait_send()
    remote(HS, HR, halo_send, halo_recv, sides[0]).wait_send()


def shards(*arrays):
    dma = pltpu.SemaphoreType.DMA
    f32 = jnp.float32
    result = pl.pallas_call(
        kernel,
        out_shape=jax.ShapeDtypeStruct((5, ROWS, COLS), f32),
        in_specs=[pl.BlockSpec(memory_space=pltpu.HBM)] * len(arrays),
        out_specs=pl.BlockSpec(memory_space=pltpu.VMEM),
        scratch_shapes=[
            pltpu.VMEM((12, 6, HEIGHT, 128), f32),
            pltpu.SMEM((NCAT,), f32),
            pltpu.VMEM((2, NCAT, ROWS, COLS), jnp.bfloat16),
            pltpu.VMEM((ROWS, COLS), jnp.int32),
            pltpu.VMEM((ROWS, COLS), jnp.int32),
            pltpu.VMEM((3, TILES, ROWS, 128), f32),
            pltpu.VMEM((3, TILES, ROWS, 128), f32),
            pltpu.VMEM((2, ROWS, 128), f32),
            pltpu.VMEM((2, ROWS, 128), f32),
            pltpu.VMEM((2, ROWS, 128), f32),
            pltpu.VMEM((2, ROWS, 128), f32),
            pltpu.VMEM((2, 16, 128), f32),
            pltpu.VMEM((2, 16, 128), f32),
            dma,
            dma((CHUNKS + 4,)),
            dma,
            dma((CHUNKS + 1,)),
            dma,
            dma,
            dma((2,)),
            dma((2,)),
            dma,
            dma,
            dma((len(LOADS),)),
            dma((len(TOPS),)),
            dma((3,)),
            pltpu.SemaphoreType.REGULAR,
        ],
        compiler_params=pltpu.CompilerParams(
            collective_id=0, has_side_effects=True, vmem_limit_bytes=44 * 2**20
        ),
        name="ice",
    )(*(pltpu.with_memory_space_constraint(a, pltpu.HBM) for a in arrays))
    return tuple(result[i] for i in range(5))


def solution(mesh):
    block = P("cat", "lat", "lon")
    plane = P("lat", "lon")
    return jax.shard_map(
        shards,
        mesh=mesh,
        in_specs=(block, block, P("cat"), *[plane] * 10),
        out_specs=(plane,) * 5,
        check_vma=False,
    )
```
